128 devices in a mesh: gx: 16 (over y, x), gy: 2 (over core), gz: 4 (over z).
Axes of the slice: x: 4, y: 4, z: 4, core: 2. Of those that a mesh axis runs over, the one named last changes fastest.
Arguments:
- potential: float32 [960, 120, 512], P('gx', 'gy', 'gz'), may hold values from -6 to 6
- frag_root: int32 [3, 512], P(None, ('gx', 'gy', 'gz')), may hold values from 0 to 959, as said below
Outputs:
- frag_fields: float32 [512, 110592], P(('gx', 'gy', 'gz'))
The draws below stay inside these ranges and needn't reach their ends.
Inputs may be any that keep to these rules, and one draw needn't show every extreme that they name: `frag_root`: fragment f is held by the device of linear index f // 4 (gx slowest). Along each dimension the box's first cell is the start of a block plus an offset in [-34, B - 34), B being that dimension's cells of one device. Along y and z that block is the holding device's own; along x it is the block of some device with the same gy and gz index, the anchor. Every anchor of a device supplies exactly 1 of its fragments.
All inputs are finite; a program needn't handle non-finite values.
Results may differ from the reference program's by a relative error of at most 0.00007.
Values sent between devices are 32-bit elements; how exact they have to be, the bound alone decides.
No kernel may reach another device: no remote copies, remote signals or barrier semaphores. Data moves between devices by JAX's collectives and lax.ppermute only.
A program may use at most 320 MiB of HBM per device.

```python
import math
import jax
import jax.numpy as jnp
from jax import lax

G = 48
CAP = 1
SLOTS = 4
BX = 60
BY = 60
BZ = 128
BOX = 68
HALO = 34
NX = 960
NY = 120
NZ = 512
N_GX = 16
N_GY = 2
N_GZ = 4


def draw_frag_root(key, part):
    subkeys = jax.random.split(jax.random.fold_in(key, 17), 6)
    devices = N_GX * N_GY * N_GZ
    pair_count = SLOTS // CAP
    favour = jax.random.randint(subkeys[0], (N_GX,), 0, 4) * 300
    jitter = jax.random.randint(subkeys[1], (devices, N_GX), 0, 1000)
    scores = (jitter + favour[None, :]) * N_GX + jnp.arange(N_GX, dtype=jnp.int32)[None, :]
    dummy_values, picked = lax.top_k(scores, pair_count)
    listed = jnp.repeat(picked.astype(jnp.int32), CAP, axis=1)
    shuffle_keys = jax.random.randint(subkeys[2], (devices, SLOTS), 0, 1000) * SLOTS + jnp.arange(SLOTS, dtype=jnp.int32)[None, :]
    shuffled = jnp.argsort(shuffle_keys, axis=1)
    anchors = jnp.take_along_axis(listed, shuffled, axis=1).reshape(-1)
    device = jnp.arange(devices * SLOTS, dtype=jnp.int32) // SLOTS
    row_y = device // N_GZ % N_GY
    row_z = device % N_GZ
    lowest = -HALO
    offset_x = jax.random.randint(subkeys[3], (devices * SLOTS,), lowest, BX - HALO)
    offset_y = jax.random.randint(subkeys[4], (devices * SLOTS,), lowest, BY - HALO)
    offset_z = jax.random.randint(subkeys[5], (devices * SLOTS,), lowest, BZ - HALO)
    offset_x = offset_x.at[0].set(lowest).at[1].set(BX - HALO - 1)
    offset_y = offset_y.at[0].set(lowest).at[1].set(BY - HALO - 1)
    offset_z = offset_z.at[0].set(lowest).at[1].set(BZ - HALO - 1)
    root_x = jnp.mod(anchors * BX + offset_x, BX * N_GX)
    root_y = jnp.mod(row_y * BY + offset_y, BY * N_GY)
    root_z = jnp.mod(row_z * BZ + offset_z, BZ * N_GZ)
    return jnp.stack([root_x, root_y, root_z]).astype(jnp.int32)


def steps_of(key, dims, pieces, smallest, top_value):
    level = 1.0
    for dim, shards_of in pieces:
        steps = jax.random.uniform(jax.random.fold_in(jax.random.fold_in(key, 6), dim), (shards_of,), jnp.float32, smallest / len(pieces), top_value / len(pieces))
        level = level * jnp.repeat(jnp.exp(steps), dims[dim] // shards_of).reshape((-1,) + (1,) * (len(dims) - 1 - dim))
    return level


def scatter_about(rng, dims, scale, most, shards=(), kind=jnp.bfloat16):
    array = scale * jax.random.normal(rng, dims, jnp.float32)
    if shards:
        array = array * steps_of(rng, dims, shards, -0.22, 0.18)
    return jnp.clip(array, -most, most).astype(kind)


def setup_inputs(seed: int = 0) -> dict:
    splits = jax.random.split(jax.random.key(seed), 3)
    potential = scatter_about(splits[0], (NX, NY, NZ), 1.0, 6.0, ((0, 16), (1, 2), (2, 4)), jnp.float32)
    frag_root = draw_frag_root(jax.random.fold_in(splits[2], 71), 0)
    return {"potential": potential, "frag_root": frag_root}


def interp_table(points, cells):
    row_index = jnp.arange(points, dtype=jnp.int32)[:, None]
    col_index = jnp.arange(cells, dtype=jnp.int32)[None, :]
    offset = row_index * cells - col_index * points
    period = points * cells
    summed = jnp.ones((points, cells), jnp.float32)
    for harmonic in range(1, points // 2):
        phase_angle = jnp.mod(harmonic * offset, period).astype(jnp.float32)
        summed = summed + 2.0 * jnp.cos((2.0 * math.pi / period) * phase_angle)
    return summed / cells


def refine(window, matrix):
    highest = lax.Precision.HIGHEST
    step_x = jnp.einsum('ax,xyz->ayz', matrix, window, precision=highest)
    step_y = jnp.einsum('by,ayz->abz', matrix, step_x, precision=highest)
    step_z = jnp.einsum('cz,abz->abc', matrix, step_y, precision=highest)
    return step_z.reshape(-1)


def reference(potential, frag_root):
    matrix = interp_table(G, BOX)
    wrapped = jnp.pad(potential, ((0, BOX), (0, BOX), (0, BOX)), mode="wrap")

    def single(corner):
        window = lax.dynamic_slice(wrapped, (corner[0], corner[1], corner[2]), (BOX, BOX, BOX))
        return refine(window, matrix)

    return lax.map(single, frag_root.T.astype(jnp.int32))
```

```python
import math

import jax
import jax.numpy as jnp
import numpy as np
from jax import lax
from jax.experimental import pallas as pl
from jax.experimental.pallas import tpu as pltpu
from jax.sharding import PartitionSpec as P


G = 48
BOX = 68
HALO = 34
NY_LOCAL = 60
YPAD = 64
ROWS = G * G * G // 128
F32 = jnp.float32
BF16 = jnp.bfloat16
ANY = pl.ANY
VMEM = pltpu.VMEM
SMEM = pltpu.SMEM

GROUPS = (
    ((0, 1), (3, 0), (1, 0), (0, 3)),
    ((2, 2), (2, 0), (0, 2), (1, 1)),
    ((3, 3), (1, 3), (3, 1), (1, 2)),
    ((2, 1), (3, 2), (2, 3), (0, 0)),
)


def interp_matrix():
    a = np.arange(G, dtype=np.float64)[:, None]
    x = np.arange(BOX, dtype=np.float64)[None, :]
    total = np.ones((G, BOX))
    for k in range(1, G // 2):
        total = total + 2.0 * np.cos(2.0 * math.pi * k * (a / G - x / BOX))
    return (total / BOX).astype(np.float32)


def vm(limit=48):
    return pltpu.CompilerParams(vmem_limit_bytes=limit << 20)


def pack_rows(p_ref, x0, n, side, i, lane):
    base = 0 if side == 0 else 128 - HALO
    rows = []
    for g in range(3):
        v = p_ref[x0 + g * n + i]
        shift = (HALO * g - base) % 128
        rows.append(pltpu.roll(v, shift, 1) if shift else v)
    return jnp.where(lane < HALO, rows[0], jnp.where(lane < 2 * HALO, rows[1], rows[2]))


def pack_kernel(p_ref, za, zb, lo_a, hi_a, lo_b, hi_b):
    lane = lax.broadcasted_iota(jnp.int32, (NY_LOCAL, 128), 1)
    for i in range(20):
        za[i] = pack_rows(p_ref, 0, 20, 0, i, lane)
        zb[i] = pack_rows(p_ref, 0, 20, 1, i, lane)
    for i in range(12):
        lo_a[i] = pack_rows(p_ref, 0, 12, 0, i, lane)
        hi_a[i] = pack_rows(p_ref, 24, 12, 0, i, lane)
        lo_b[i] = pack_rows(p_ref, 0, 12, 1, i, lane)
        hi_b[i] = pack_rows(p_ref, 24, 12, 1, i, lane)


def pack(p):
    big = jax.ShapeDtypeStruct((20, NY_LOCAL, 128), F32)
    small = jax.ShapeDtypeStruct((12, NY_LOCAL, 128), F32)
    return pl.pallas_call(
        pack_kernel,
        out_shape=(big, big, small, small, small, small),
        compiler_params=vm(),
        name="pack",
    )(p)


def turn(src, out, count):
    for y in range(NY_LOCAL):
        out[:, y, :] = src[:, y, :].T[:count]
    out[:, NY_LOCAL:, :] = jnp.zeros((count, YPAD - NY_LOCAL, 128), F32)


def mid_kernel(before, own, after, out, x_ref, sems):
    copies = [
        pltpu.make_async_copy(before, x_ref.at[pl.ds(0, HALO)], sems.at[0]),
        pltpu.make_async_copy(own, x_ref.at[pl.ds(HALO, 60)], sems.at[1]),
        pltpu.make_async_copy(after, x_ref.at[pl.ds(HALO + 60, HALO)], sems.at[2]),
    ]
    for c in copies:
        c.start()
    for c in copies:
        c.wait()
    turn(x_ref, out, 128)


def middle(before, own, after):
    return pl.pallas_call(
        mid_kernel,
        out_shape=jax.ShapeDtypeStruct((128, YPAD, 128), F32),
        in_specs=[pl.BlockSpec(memory_space=ANY)] * 3,
        scratch_shapes=[VMEM((128, NY_LOCAL, 128), F32), pltpu.SemaphoreType.DMA((3,))],
        compiler_params=vm(),
        name="middle",
    )(before, own, after)


def halo_kernel(zb, za, lb, la, rb, ra, out, x_ref):
    lane = lax.broadcasted_iota(jnp.int32, (NY_LOCAL, 128), 1)

    def place(b_ref, a_ref, i, g, row):
        b = b_ref[i]
        a = a_ref[i]
        sb = (-HALO * g) % 128
        sa = (40 - HALO * g) % 128
        b = pltpu.roll(b, sb, 1) if sb else b
        a = pltpu.roll(a, sa, 1) if sa else a
        x_ref[row] = jnp.where(lane < 40, b, a)

    for g in range(3):
        for i in range(20):
            place(zb, za, i, g, HALO + 20 * g + i)
        for i in range(12):
            x = 12 * g + i - 2
            if x >= 0:
                place(lb, la, i, g, x)
            x = 12 * g + i
            if x < HALO:
                place(rb, ra, i, g, HALO + 60 + x)
    turn(x_ref, out, 80)


def halos(zb, za, lb, la, rb, ra):
    return pl.pallas_call(
        halo_kernel,
        out_shape=jax.ShapeDtypeStruct((80, YPAD, 128), F32),
        scratch_shapes=[VMEM((128, NY_LOCAL, 128), F32)],
        compiler_params=vm(),
        name="halos",
    )(zb, za, lb, la, rb, ra)


def split_rows(f):
    hi = f.astype(BF16).astype(F32)
    return jnp.concatenate([hi, f - hi], axis=0).astype(BF16)


def placed(table_hi, table_lo, hot):
    hot = jnp.where(hot, 1.0, 0.0).astype(BF16)
    hi = jnp.dot(table_hi, hot, preferred_element_type=F32)
    lo = jnp.dot(table_lo, hot, preferred_element_type=F32)
    top = jnp.concatenate([hi, hi], axis=1)
    low = jnp.concatenate([lo, jnp.zeros_like(lo)], axis=1)
    return jnp.concatenate([top, low], axis=0).astype(BF16)


def folded(r):
    return r[:G] + r[G:]


def locate(roots, place, sizes, slot, holder):
    nx, ny, nz, bx, by, bz = sizes
    ok = jnp.int32(0)
    x0 = y0 = z0 = jnp.int32(0)
    for s in range(slot):
        def rel(dim, origin, total):
            v = roots[dim, holder * slot + s] + HALO - origin
            return jnp.where(v < 0, v + total, jnp.where(v >= total, v - total, v))
        rx = rel(0, place[0] * bx, nx)
        mine = rx < bx
        ok = jnp.where(mine, 1, ok)
        x0 = jnp.where(mine, rx, x0)
        y0 = jnp.where(mine, rel(1, place[1] * by, ny) - HALO, y0)
        z0 = jnp.where(mine, rel(2, place[2] * bz, nz), z0)
    return ok, x0, y0, z0


def field_kernel(shifts, sizes, slot, roots, place, thi, tlo, a2_ref, own_m, part_m, own_h, part_h, *rest):
    n = len(shifts)
    outs = rest[:n]
    w_own, w_part, t1, t2, obuf, info, in_sems, out_sems = rest[n:]
    gx = place[0]
    py = gx // 4
    px = gx % 4

    for j, (dy, dx) in enumerate(shifts):
        holder = ((py + dy) % 4) * 4 + (px + dx) % 4
        ok, x0, y0, z0 = locate(roots, place, sizes, slot, holder)
        info[0, j] = ok
        info[1, j] = x0
        info[2, j] = y0
        info[3, j] = z0
    info[0, n] = jnp.int32(0)

    def copies(j, b):
        z0 = info[3, j]
        c = jnp.clip(z0 - HALO, 0, 128 - BOX)
        for k, (src_m, src_h, w) in enumerate(((own_m, own_h, w_own), (part_m, part_h, w_part))):
            yield None, pltpu.make_async_copy(
                src_m.at[pl.ds(c, BOX)], w.at[b, pl.ds(HALO, BOX)], in_sems.at[b, 2 * k])
            yield z0 < HALO, pltpu.make_async_copy(
                src_h.at[pl.ds(0, HALO)], w.at[b, pl.ds(0, HALO)], in_sems.at[b, 2 * k + 1])
            yield z0 > 128 - HALO, pltpu.make_async_copy(
                src_h.at[pl.ds(40, HALO)], w.at[b, pl.ds(HALO + BOX, HALO)], in_sems.at[b, 2 * k + 1])

    def begin(j, b):
        for cond, c in copies(j, b):
            if cond is None:
                c.start()
            else:
                pl.when(cond)(c.start)

    def finish(j, b):
        for cond, c in copies(j, b):
            if cond is None:
                c.wait()
            else:
                pl.when(cond)(c.wait)

    def out_copy(k, b):
        return pltpu.make_async_copy(obuf.at[b], outs[k], out_sems.at[b])

    for b in range(G):
        t1[b * 72 + 64:b * 72 + 72, :] = jnp.zeros((8, 128), F32)

    def compute(j, b):
        x0 = info[1, j]
        y0 = info[2, j]
        z0 = info[3, j]
        zoff = z0 - jnp.clip(z0 - HALO, 0, 128 - BOX)
        k = lax.broadcasted_iota(jnp.int32, (128, 128), 0)
        col = lax.broadcasted_iota(jnp.int32, (128, 128), 1)
        half = col & 63
        near = jnp.where(col < 64, col, col - 4) - y0
        far = jnp.where(col < 64, -1, col - 124 - y0)
        hot_y = jnp.logical_and(half < NY_LOCAL, jnp.logical_or(k == near, k == far))
        a1 = placed(thi[...], tlo[...], hot_y)
        a3 = placed(thi[...], tlo[...], k == col - x0)
        a2 = a2_ref[...]
        for p in range(BOX // 2):
            z = zoff + 2 * p
            own = jnp.concatenate([w_own[b, z], w_own[b, z + 1]], axis=1)
            part = jnp.concatenate([w_part[b, z], w_part[b, z + 1]], axis=1)
            rhs = split_rows(jnp.concatenate([own, part], axis=0))
            t = folded(jnp.dot(a1, rhs, preferred_element_type=F32))
            t1[pl.ds(2 * p, G, stride=72), :] = t[:, :128]
            t1[pl.ds(2 * p + 1, G, stride=72), :] = t[:, 128:]
        for q in range(0, G, 2):
            f = jnp.concatenate([t1[q * 72:q * 72 + 72, :], t1[q * 72 + 72:q * 72 + 144, :]], axis=1)
            t = folded(jnp.dot(a2, split_rows(f), preferred_element_type=F32))
            t2[q * G:q * G + G, :] = t[:, :128]
            t2[q * G + G:q * G + 2 * G, :] = t[:, 128:]
        for m in range(9):
            f = t2[256 * m:256 * m + 256, :]
            hi = f.astype(BF16)
            lo = (f - hi.astype(F32)).astype(BF16)
            rhs = jnp.concatenate([hi, lo], axis=1)
            r = lax.dot_general(a3, rhs, (((1,), (1,)), ((), ())), preferred_element_type=F32)
            t = folded(r)
            obuf[b, pl.ds(2 * m, G, stride=18), :] = t[:, :128]
            obuf[b, pl.ds(2 * m + 1, G, stride=18), :] = t[:, 128:]

    @pl.when(info[0, 0] == 1)
    def _():
        begin(0, 0)

    def step(j, carry):
        b = lax.rem(j, 2)

        @pl.when(info[0, j + 1] == 1)
        def _():
            begin(j + 1, 1 - b)

        @pl.when(info[0, j] == 1)
        def _():
            finish(j, b)
            compute(j, b)
            for k in range(n):
                @pl.when(j == k)
                def _(k=k):
                    out_copy(k, b).start()
            out_copy(0, b).wait()

        return carry

    lax.fori_loop(0, n, step, 0)


def fields(shifts, sizes, slot, roots, place, thi, tlo, a2, own_m, part_m, own_h, part_h):
    n = len(shifts)
    out = jax.ShapeDtypeStruct((ROWS, 128), F32)
    smem = pl.BlockSpec(memory_space=SMEM)
    vmem = pl.BlockSpec(memory_space=VMEM)
    hbm = pl.BlockSpec(memory_space=ANY)

    def kernel(*refs):
        field_kernel(shifts, sizes, slot, *refs)

    return pl.pallas_call(
        kernel,
        out_shape=(out,) * n,
        in_specs=[smem, smem, vmem, vmem, vmem, hbm, hbm, hbm, hbm],
        out_specs=(hbm,) * n,
        scratch_shapes=[
            VMEM((2, 2 * HALO + BOX, YPAD, 128), F32),
            VMEM((2, 2 * HALO + BOX, YPAD, 128), F32),
            VMEM((G * 72, 128), F32),
            VMEM((G * G, 128), F32),
            VMEM((2, ROWS, 128), F32),
            SMEM((4, n + 1), jnp.int32),
            pltpu.SemaphoreType.DMA((2, 4)),
            pltpu.SemaphoreType.DMA((2,)),
        ],
        compiler_params=vm(),
        cost_estimate=pl.CostEstimate(flops=2_000_000_000 * n, bytes_accessed=5_000_000 * n, transcendentals=0),
        name="fields",
    )(roots, place, thi, tlo, a2, own_m, part_m, own_h, part_h)


def pick_kernel(order, sizes, slot, own_root, place, *rest):
    srcs = rest[:16]
    out, buf, sems = rest[16:]
    nx, bx = sizes[0], sizes[3]
    gx = place[0]
    py = gx // 4
    px = gx % 4
    for s in range(slot):
        r = own_root[0, s] + HALO
        for k, (dy, dx) in enumerate(order):
            anchor = ((py + 4 - dy) % 4) * 4 + (px + 4 - dx) % 4
            v = r - anchor * bx
            v = jnp.where(v < 0, v + nx, jnp.where(v >= nx, v - nx, v))

            @pl.when(v < bx)
            def _(k=k, s=s):
                pltpu.make_async_copy(srcs[k], buf.at[s], sems.at[s]).start()
    for s in range(slot):
        pltpu.make_async_copy(srcs[0], buf.at[s], sems.at[s]).wait()
        out[:, s, :] = buf[s]


def pick(order, sizes, slot, own_root, place, parts):
    smem = pl.BlockSpec(memory_space=SMEM)

    def kernel(*refs):
        pick_kernel(order, sizes, slot, *refs)

    return pl.pallas_call(
        kernel,
        out_shape=jax.ShapeDtypeStruct((ROWS, slot, 128), F32),
        in_specs=[smem, smem] + [pl.BlockSpec(memory_space=ANY)] * 16,
        scratch_shapes=[VMEM((slot, ROWS, 128), F32), pltpu.SemaphoreType.DMA((slot,))],
        compiler_params=vm(),
        name="pick",
    )(own_root, place, *parts)


def body(potential, frag_root):
    bx, by, bz = potential.shape
    groups = lax.axis_size("gx")
    zs = lax.axis_size("gz")
    sizes = (bx * groups, by * lax.axis_size("gy"), bz * zs, bx, by, bz)
    slot = frag_root.shape[1]
    place = jnp.stack([lax.axis_index("gx"), lax.axis_index("gy"), lax.axis_index("gz")]).astype(jnp.int32)

    def move(v, sx, sz):
        if sz == 0:
            return lax.ppermute(v, "gx", [(i, (i + sx) % groups) for i in range(groups)])
        if sx == 0:
            return lax.ppermute(v, "gz", [(i, (i + sz) % zs) for i in range(zs)])
        perm = []
        for i in range(groups):
            for j in range(zs):
                perm.append((i * zs + j, ((i + sx) % groups) * zs + (j + sz) % zs))
        return lax.ppermute(v, ("gx", "gz"), perm)

    before = move(potential[bx - HALO:], 1, 0)
    after = move(potential[:HALO], -1, 0)
    za, zb, lo_a, hi_a, lo_b, hi_b = pack(potential)
    got_zb = move(zb, 0, 1)
    got_za = move(za, 0, -1)
    got_lb = move(hi_b, 1, 1)
    got_rb = move(lo_b, -1, 1)
    got_la = move(hi_a, 1, -1)
    got_ra = move(lo_a, -1, -1)
    roots = lax.all_gather(frag_root, "gx", axis=1, tiled=True)

    swap = [(0, 1), (1, 0)]
    own_m = middle(before, potential, after)
    part_m = lax.ppermute(own_m, "gy", swap)
    own_h = halos(got_zb, got_za, got_lb, got_la, got_rb, got_ra)
    part_h = lax.ppermute(own_h, "gy", swap)

    table = interp_matrix()
    hi = np.asarray(table.astype(BF16))
    lo = (table - hi.astype(np.float32)).astype(BF16)
    thi = np.zeros((G, 128), BF16)
    tlo = np.zeros((G, 128), BF16)
    thi[:, :BOX] = hi
    tlo[:, :BOX] = lo
    a2 = np.zeros((2 * G, 144), BF16)
    a2[:G, :BOX] = hi
    a2[:G, 72:72 + BOX] = hi
    a2[G:, :BOX] = lo

    order = []
    parts = []
    for shifts in GROUPS:
        done = fields(shifts, sizes, slot, roots, place, thi, tlo, a2, own_m, part_m, own_h, part_h)
        for (dy, dx), v in zip(shifts, done):
            order.append((dy, dx))
            if (dy, dx) != (0, 0):
                perm = [(4 * y + x, 4 * ((y + dy) % 4) + (x + dx) % 4) for y in range(4) for x in range(4)]
                v = lax.ppermute(v, "gx", perm)
            parts.append(v)
    out = pick(tuple(order), sizes, slot, frag_root, place, parts)
    return jnp.transpose(out, (1, 0, 2)).reshape(slot, ROWS * 128)


def solution(mesh):
    return jax.shard_map(
        body,
        mesh=mesh,
        in_specs=(P("gx", "gy", "gz"), P(None, ("gx", "gy", "gz"))),
        out_specs=P(("gx", "gy", "gz"), None),
        check_vma=False,
    )
```

```python
import math

import jax
import jax.numpy as jnp
import numpy as np
from jax import lax
from jax.experimental import pallas as pl
from jax.experimental.pallas import tpu as pltpu
from jax.sharding import PartitionSpec as P


G = 48
BOX = 68
HALO = 34
NY_LOCAL = 60
YPAD = 64
ROWS = G * G * G // 128
F32 = jnp.float32
BF16 = jnp.bfloat16
MID_COST = 10
FIELD_COST = 3
ANY = pl.ANY
VMEM = pltpu.VMEM
SMEM = pltpu.SMEM

GROUPS = (
    ((0, 1), (3, 0), (1, 0), (0, 3)),
    ((2, 2), (2, 0), (0, 2), (1, 1)),
    ((3, 3), (1, 3), (3, 1), (1, 2)),
    ((2, 1), (3, 2), (2, 3), (0, 0)),
)


def interp_matrix():
    a = np.arange(G, dtype=np.float64)[:, None]
    x = np.arange(BOX, dtype=np.float64)[None, :]
    total = np.ones((G, BOX))
    for k in range(1, G // 2):
        total = total + 2.0 * np.cos(2.0 * math.pi * k * (a / G - x / BOX))
    return (total / BOX).astype(np.float32)


def cost(us):
    return pl.CostEstimate(flops=int(us * 1e9), bytes_accessed=0, transcendentals=0)


def vm(limit=48):
    return pltpu.CompilerParams(vmem_limit_bytes=limit << 20)


def pack_rows(p_ref, x0, n, side, i, lane):
    base, first = (0, 40) if side == 0 else (128 - HALO, 0)
    rows = []
    for g in range(3):
        v = p_ref[x0 + g * n + i]
        shift = (first + HALO * g - base) % 128
        rows.append(pltpu.roll(v, shift, 1) if shift else v)
    at = jnp.where(lane < first, lane + 128 - first, lane - first)
    return jnp.where(at < HALO, rows[0], jnp.where(at < 2 * HALO, rows[1], rows[2]))


def pack_kernel(p_ref, za, zb, lo_a, hi_a, lo_b, hi_b):
    lane = lax.broadcasted_iota(jnp.int32, (NY_LOCAL, 128), 1)
    for i in range(20):
        za[i] = pack_rows(p_ref, 0, 20, 0, i, lane)
        zb[i] = pack_rows(p_ref, 0, 20, 1, i, lane)
    for i in range(12):
        lo_a[i] = pack_rows(p_ref, 0, 12, 0, i, lane)
        hi_a[i] = pack_rows(p_ref, 24, 12, 0, i, lane)
        lo_b[i] = pack_rows(p_ref, 0, 12, 1, i, lane)
        hi_b[i] = pack_rows(p_ref, 24, 12, 1, i, lane)


def pack(p):
    big = jax.ShapeDtypeStruct((20, NY_LOCAL, 128), F32)
    small = jax.ShapeDtypeStruct((12, NY_LOCAL, 128), F32)
    return pl.pallas_call(
        pack_kernel,
        out_shape=(big, big, small, small, small, small),
        compiler_params=vm(),
        name="pack",
    )(p)


def turn(src, out, count):
    for y in range(NY_LOCAL):
        out[:, y, :] = src[:, y, :].T[:count]
    out[:, NY_LOCAL:, :] = jnp.zeros((count, YPAD - NY_LOCAL, 128), F32)


def mid_kernel(before, own, after, packed, out, x_ref, sems):
    copies = [
        pltpu.make_async_copy(before, x_ref.at[pl.ds(0, HALO)], sems.at[0]),
        pltpu.make_async_copy(own, x_ref.at[pl.ds(HALO, 60)], sems.at[1]),
        pltpu.make_async_copy(after, x_ref.at[pl.ds(HALO + 60, HALO)], sems.at[2]),
    ]
    for c in copies:
        c.start()
    for c in copies:
        c.wait()
    turn(x_ref, out, 128)


def middle(before, own, after, packed):
    return pl.pallas_call(
        mid_kernel,
        out_shape=jax.ShapeDtypeStruct((128, YPAD, 128), F32),
        in_specs=[pl.BlockSpec(memory_space=ANY)] * 4,
        scratch_shapes=[VMEM((128, NY_LOCAL, 128), F32), pltpu.SemaphoreType.DMA((3,))],
        compiler_params=vm(),
        cost_estimate=cost(MID_COST),
        name="middle",
    )(before, own, after, packed)


def halo_kernel(zb, za, lb, la, rb, ra, roots, out, x_ref):
    lane = lax.broadcasted_iota(jnp.int32, (NY_LOCAL, 128), 1)

    def place(b_ref, a_ref, i, g, row):
        mine = jnp.logical_and(lane >= HALO * g, lane < HALO * g + HALO)
        v = jnp.where(mine, b_ref[i], a_ref[i])
        x_ref[row] = pltpu.roll(v, 128 - HALO * g, 1) if g else v

    for g in range(3):
        for i in range(20):
            place(zb, za, i, g, HALO + 20 * g + i)
        for i in range(12):
            x = 12 * g + i - 2
            if x >= 0:
                place(lb, la, i, g, x)
            x = 12 * g + i
            if x < HALO:
                place(rb, ra, i, g, HALO + 60 + x)
    turn(x_ref, out, 80)


def halos(zb, za, lb, la, rb, ra, roots):
    return pl.pallas_call(
        halo_kernel,
        out_shape=jax.ShapeDtypeStruct((80, YPAD, 128), F32),
        in_specs=[pl.BlockSpec(memory_space=VMEM)] * 6 + [pl.BlockSpec(memory_space=SMEM)],
        scratch_shapes=[VMEM((128, NY_LOCAL, 128), F32)],
        compiler_params=vm(),
        cost_estimate=cost(5),
        name="halos",
    )(zb, za, lb, la, rb, ra, roots)


def split_rows(f):
    hi = f.astype(BF16).astype(F32)
    return jnp.concatenate([hi, f - hi], axis=0).astype(BF16)


def placed(table_hi, table_lo, hot):
    hot = jnp.where(hot, 1.0, 0.0).astype(BF16)
    hi = jnp.dot(table_hi, hot, preferred_element_type=F32)
    lo = jnp.dot(table_lo, hot, preferred_element_type=F32)
    top = jnp.concatenate([hi, hi], axis=1)
    low = jnp.concatenate([lo, jnp.zeros_like(lo)], axis=1)
    return jnp.concatenate([top, low], axis=0).astype(BF16)


def folded(r):
    return r[:G] + r[G:]


def locate(roots, place, sizes, slot, holder):
    nx, ny, nz, bx, by, bz = sizes
    ok = jnp.int32(0)
    x0 = y0 = z0 = jnp.int32(0)
    for s in range(slot):
        def rel(dim, origin, total):
            v = roots[holder, dim, s] + HALO - origin
            return jnp.where(v < 0, v + total, jnp.where(v >= total, v - total, v))

        rx = rel(0, place[0] * bx, nx)
        mine = rx < bx
        ok = jnp.where(mine, 1, ok)
        x0 = jnp.where(mine, rx, x0)
        y0 = jnp.where(mine, rel(1, place[1] * by, ny) - HALO, y0)
        z0 = jnp.where(mine, rel(2, place[2] * bz, nz), z0)
    return ok, x0, y0, z0


def field_kernel(shifts, sizes, slot, roots, place, thi, tlo, a2_ref, own_m, part_m, own_h, part_h, *rest):
    n = len(shifts)
    outs = rest[:n]
    w_own, w_part, t1, t2, obuf, info, in_sems, out_sems = rest[n:]
    gx = place[0]
    py = gx // 4
    px = gx % 4

    for j, (dy, dx) in enumerate(shifts):
        holder = ((py + dy) % 4) * 4 + (px + dx) % 4
        ok, x0, y0, z0 = locate(roots, place, sizes, slot, holder)
        info[0, j] = ok
        info[1, j] = x0
        info[2, j] = y0
        info[3, j] = z0
    info[0, n] = jnp.int32(0)

    def copies(j, b):
        z0 = info[3, j]
        c = jnp.clip(z0 - HALO, 0, 128 - BOX)
        for k, (src_m, src_h, w) in enumerate(((own_m, own_h, w_own), (part_m, part_h, w_part))):
            yield None, pltpu.make_async_copy(
                src_m.at[pl.ds(c, BOX)], w.at[b, pl.ds(HALO, BOX)], in_sems.at[b, 2 * k])
            yield z0 < HALO, pltpu.make_async_copy(
                src_h.at[pl.ds(0, HALO)], w.at[b, pl.ds(0, HALO)], in_sems.at[b, 2 * k + 1])
            yield z0 > 128 - HALO, pltpu.make_async_copy(
                src_h.at[pl.ds(40, HALO)], w.at[b, pl.ds(HALO + BOX, HALO)], in_sems.at[b, 2 * k + 1])

    def begin(j, b):
        for cond, c in copies(j, b):
            if cond is None:
                c.start()
            else:
                pl.when(cond)(c.start)

    def finish(j, b):
        for cond, c in copies(j, b):
            if cond is None:
                c.wait()
            else:
                pl.when(cond)(c.wait)

    def out_copy(k, b):
        return pltpu.make_async_copy(obuf.at[b], outs[k], out_sems.at[b])

    for b in range(G):
        t1[b * 72 + 64:b * 72 + 72, :] = jnp.zeros((8, 128), F32)

    def compute(j, b):
        x0 = info[1, j]
        y0 = info[2, j]
        z0 = info[3, j]
        zoff = z0 - jnp.clip(z0 - HALO, 0, 128 - BOX)
        k = lax.broadcasted_iota(jnp.int32, (128, 128), 0)
        col = lax.broadcasted_iota(jnp.int32, (128, 128), 1)
        half = col & 63
        near = jnp.where(col < 64, col, col - 4) - y0
        far = jnp.where(col < 64, -1, col - 124 - y0)
        hot_y = jnp.logical_and(half < NY_LOCAL, jnp.logical_or(k == near, k == far))
        a1 = placed(thi[...], tlo[...], hot_y)
        a3 = placed(thi[...], tlo[...], k == col - x0)
        a2 = a2_ref[...]
        for p in range(BOX // 2):
            z = zoff + 2 * p
            own = jnp.concatenate([w_own[b, z], w_own[b, z + 1]], axis=1)
            part = jnp.concatenate([w_part[b, z], w_part[b, z + 1]], axis=1)
            rhs = split_rows(jnp.concatenate([own, part], axis=0))
            t = folded(jnp.dot(a1, rhs, preferred_element_type=F32))
            t1[pl.ds(2 * p, G, stride=72), :] = t[:, :128]
            t1[pl.ds(2 * p + 1, G, stride=72), :] = t[:, 128:]
        for q in range(0, G, 2):
            f = jnp.concatenate([t1[q * 72:q * 72 + 72, :], t1[q * 72 + 72:q * 72 + 144, :]], axis=1)
            t = folded(jnp.dot(a2, split_rows(f), preferred_element_type=F32))
            t2[q * G:q * G + G, :] = t[:, :128]
            t2[q * G + G:q * G + 2 * G, :] = t[:, 128:]
        for m in range(9):
            f = t2[256 * m:256 * m + 256, :]
            hi = f.astype(BF16)
            lo = (f - hi.astype(F32)).astype(BF16)
            rhs = jnp.concatenate([hi, lo], axis=1)
            r = lax.dot_general(a3, rhs, (((1,), (1,)), ((), ())), preferred_element_type=F32)
            t = folded(r)
            obuf[b, pl.ds(2 * m, G, stride=18), :] = t[:, :128]
            obuf[b, pl.ds(2 * m + 1, G, stride=18), :] = t[:, 128:]

    @pl.when(info[0, 0] == 1)
    def _():
        begin(0, 0)

    def step(j, carry):
        b = lax.rem(j, 2)

        @pl.when(info[0, j + 1] == 1)
        def _():
            begin(j + 1, 1 - b)

        @pl.when(info[0, j] == 1)
        def _():
            finish(j, b)
            compute(j, b)
            for k in range(n):
                @pl.when(j == k)
                def _(k=k):
                    out_copy(k, b).start()
            out_copy(0, b).wait()

        return carry

    lax.fori_loop(0, n, step, 0)


def fields(shifts, sizes, slot, roots, place, thi, tlo, a2, own_m, part_m, own_h, part_h):
    n = len(shifts)
    out = jax.ShapeDtypeStruct((ROWS, 128), F32)
    smem = pl.BlockSpec(memory_space=SMEM)
    vmem = pl.BlockSpec(memory_space=VMEM)
    hbm = pl.BlockSpec(memory_space=ANY)

    def kernel(*refs):
        field_kernel(shifts, sizes, slot, *refs)

    return pl.pallas_call(
        kernel,
        out_shape=(out,) * n,
        in_specs=[smem, smem, vmem, vmem, vmem, hbm, hbm, hbm, hbm],
        out_specs=(hbm,) * n,
        scratch_shapes=[
            VMEM((2, 2 * HALO + BOX, YPAD, 128), F32),
            VMEM((2, 2 * HALO + BOX, YPAD, 128), F32),
            VMEM((G * 72, 128), F32),
            VMEM((G * G, 128), F32),
            VMEM((2, ROWS, 128), F32),
            SMEM((4, n + 1), jnp.int32),
            pltpu.SemaphoreType.DMA((2, 4)),
            pltpu.SemaphoreType.DMA((2,)),
        ],
        compiler_params=vm(),
        cost_estimate=cost(FIELD_COST * n),
        name="fields",
    )(roots, place, thi, tlo, a2, own_m, part_m, own_h, part_h)


def pick_kernel(order, sizes, slot, own_root, place, *rest):
    srcs = rest[:16]
    out, buf, sems = rest[16:]
    nx, bx = sizes[0], sizes[3]
    gx = place[0]
    py = gx // 4
    px = gx % 4
    for s in range(slot):
        r = own_root[0, s] + HALO
        for k, (dy, dx) in enumerate(order):
            anchor = ((py + 4 - dy) % 4) * 4 + (px + 4 - dx) % 4
            v = r - anchor * bx
            v = jnp.where(v < 0, v + nx, jnp.where(v >= nx, v - nx, v))

            @pl.when(v < bx)
            def _(k=k, s=s):
                pltpu.make_async_copy(srcs[k], buf.at[s], sems.at[s]).start()
    for s in range(slot):
        pltpu.make_async_copy(srcs[0], buf.at[s], sems.at[s]).wait()
        out[:, s, :] = buf[s]


def pick(order, sizes, slot, own_root, place, parts):
    smem = pl.BlockSpec(memory_space=SMEM)

    def kernel(*refs):
        pick_kernel(order, sizes, slot, *refs)

    return pl.pallas_call(
        kernel,
        out_shape=jax.ShapeDtypeStruct((ROWS, slot, 128), F32),
        in_specs=[smem, smem] + [pl.BlockSpec(memory_space=ANY)] * 16,
        scratch_shapes=[VMEM((slot, ROWS, 128), F32), pltpu.SemaphoreType.DMA((slot,))],
        compiler_params=vm(),
        name="pick",
    )(own_root, place, *parts)


def program(potential, frag_root):
    bx, by, bz = potential.shape
    groups = lax.axis_size("gx")
    zs = lax.axis_size("gz")
    sizes = (bx * groups, by * lax.axis_size("gy"), bz * zs, bx, by, bz)
    slot = frag_root.shape[1]
    place = jnp.stack([lax.axis_index("gx"), lax.axis_index("gy"), lax.axis_index("gz")]).astype(jnp.int32)

    def moved(v, sx, sz):
        if sz == 0:
            return lax.ppermute(v, "gx", [(i, (i + sx) % groups) for i in range(groups)])
        if sx == 0:
            return lax.ppermute(v, "gz", [(i, (i + sz) % zs) for i in range(zs)])
        perm = []
        for i in range(groups):
            for j in range(zs):
                perm.append((i * zs + j, ((i + sx) % groups) * zs + (j + sz) % zs))
        return lax.ppermute(v, ("gx", "gz"), perm)

    before = moved(potential[bx - HALO:], 1, 0)
    after = moved(potential[:HALO], -1, 0)
    za, zb, lo_a, hi_a, lo_b, hi_b = pack(potential)
    got_zb = moved(zb, 0, 1)
    got_za = moved(za, 0, -1)
    got_lb = moved(hi_b, 1, 1)
    got_rb = moved(lo_b, -1, 1)
    got_la = moved(hi_a, 1, -1)
    got_ra = moved(lo_a, -1, -1)
    roots = lax.all_to_all(
        jnp.broadcast_to(frag_root[None], (groups, 3, slot)), "gx", 0, 0, tiled=True
    )

    swap = [(0, 1), (1, 0)]
    own_m = middle(before, potential, after, zb)
    part_m = lax.ppermute(own_m, "gy", swap)
    own_h = halos(got_zb, got_za, got_lb, got_la, got_rb, got_ra, roots)
    part_h = lax.ppermute(own_h, "gy", swap)

    table = interp_matrix()
    hi = np.asarray(table.astype(BF16))
    lo = (table - hi.astype(np.float32)).astype(BF16)
    thi = np.zeros((G, 128), BF16)
    tlo = np.zeros((G, 128), BF16)
    thi[:, :BOX] = hi
    tlo[:, :BOX] = lo
    a2 = np.zeros((2 * G, 144), BF16)
    a2[:G, :BOX] = hi
    a2[:G, 72:72 + BOX] = hi
    a2[G:, :BOX] = lo

    order = []
    parts = []
    for shifts in GROUPS:
        done = fields(shifts, sizes, slot, roots, place, thi, tlo, a2, own_m, part_m, own_h, part_h)
        for (dy, dx), v in zip(shifts, done):
            order.append((dy, dx))
            if (dy, dx) != (0, 0):
                perm = [(4 * y + x, 4 * ((y + dy) % 4) + (x + dx) % 4) for y in range(4) for x in range(4)]
                v = lax.ppermute(v, "gx", perm)
            parts.append(v)
    out = pick(tuple(order), sizes, slot, frag_root, place, parts)
    return jnp.transpose(out, (1, 0, 2)).reshape(slot, ROWS * 128)


def solution(mesh):
    return jax.shard_map(
        program,
        mesh=mesh,
        in_specs=(P("gx", "gy", "gz"), P(None, ("gx", "gy", "gz"))),
        out_specs=P(("gx", "gy", "gz"), None),
        check_vma=False,
    )
```

```python
import math

import jax
import jax.numpy as jnp
import numpy as np
from jax import lax
from jax.experimental import pallas as pl
from jax.experimental.pallas import tpu as pltpu
from jax.sharding import PartitionSpec as P


G = 48
BOX = 68
HALO = 34
NY_LOCAL = 60
YPAD = 64
ROWS = G * G * G // 128
F32 = jnp.float32
BF16 = jnp.bfloat16
MID_COST = 10
FIELD_COST = 3
ANY = pl.ANY
VMEM = pltpu.VMEM
SMEM = pltpu.SMEM

GROUPS = (
    ((1, 2), (3, 2), (2, 1), (2, 3)),
    ((1, 1), (3, 3), (1, 3), (3, 1), (2, 2)),
    ((0, 1), (0, 3), (1, 0), (3, 0), (0, 2), (2, 0), (0, 0)),
)


def interp_matrix():
    a = np.arange(G, dtype=np.float64)[:, None]
    x = np.arange(BOX, dtype=np.float64)[None, :]
    total = np.ones((G, BOX))
    for k in range(1, G // 2):
        total = total + 2.0 * np.cos(2.0 * math.pi * k * (a / G - x / BOX))
    return (total / BOX).astype(np.float32)


def cost(us):
    return pl.CostEstimate(flops=int(us * 1e9), bytes_accessed=0, transcendentals=0)


def vm(limit=48):
    return pltpu.CompilerParams(vmem_limit_bytes=limit << 20)


def pack_rows(p_ref, side, i, lane):
    base, first = (0, 40) if side == 0 else (128 - HALO, 0)
    rows = []
    for g in range(3):
        v = p_ref[3 * i + g]
        shift = (first + HALO * g - base) % 128
        rows.append(pltpu.roll(v, shift, 1) if shift else v)
    at = jnp.where(lane < first, lane + 128 - first, lane - first)
    return jnp.where(at < HALO, rows[0], jnp.where(at < 2 * HALO, rows[1], rows[2]))


def pack_kernel(p_ref, za, zb):
    lane = lax.broadcasted_iota(jnp.int32, (NY_LOCAL, 128), 1)
    for i in range(20):
        za[i, :NY_LOCAL] = pack_rows(p_ref, 0, i, lane)
        zb[i, :NY_LOCAL] = pack_rows(p_ref, 1, i, lane)


def pack(p):
    big = jax.ShapeDtypeStruct((20, YPAD, 128), F32)
    return pl.pallas_call(
        pack_kernel,
        out_shape=(big, big),
        compiler_params=vm(16),
        name="pack",
    )(p)


def turn(src, out, count):
    for y in range(NY_LOCAL):
        out[:, y, :] = src[:, y, :].T[:count]
    out[:, NY_LOCAL:, :] = jnp.zeros((count, YPAD - NY_LOCAL, 128), F32)


def mid_kernel(before, own, after, packed, out, x_ref, sems):
    copies = [
        pltpu.make_async_copy(before, x_ref.at[pl.ds(0, HALO)], sems.at[0]),
        pltpu.make_async_copy(own, x_ref.at[pl.ds(HALO, 60)], sems.at[1]),
        pltpu.make_async_copy(after, x_ref.at[pl.ds(HALO + 60, HALO)], sems.at[2]),
    ]
    for c in copies:
        c.start()
    for c in copies:
        c.wait()
    turn(x_ref, out, 128)


def middle(before, own, after, packed):
    return pl.pallas_call(
        mid_kernel,
        out_shape=jax.ShapeDtypeStruct((128, YPAD, 128), F32),
        in_specs=[pl.BlockSpec(memory_space=ANY)] * 4,
        scratch_shapes=[VMEM((128, NY_LOCAL, 128), F32), pltpu.SemaphoreType.DMA((3,))],
        compiler_params=vm(20),
        cost_estimate=cost(MID_COST),
        name="middle",
    )(before, own, after, packed)


def halo_kernel(zb, za, left, right, roots, out, x_ref):
    lane = lax.broadcasted_iota(jnp.int32, (NY_LOCAL, 128), 1)

    def place(b, a, g, row):
        mine = jnp.logical_and(lane >= HALO * g, lane < HALO * g + HALO)
        v = jnp.where(mine, b, a)
        x_ref[row] = pltpu.roll(v, 128 - HALO * g, 1) if g else v

    for g in range(3):
        for i in range(20):
            place(zb[i, :NY_LOCAL], za[i, :NY_LOCAL], g, HALO + 3 * i + g)
        for i in range(12):
            x = 3 * i + g - 2
            if x >= 0:
                place(left[i, :NY_LOCAL], left[12 + i, :NY_LOCAL], g, x)
            x = 3 * i + g
            if x < HALO:
                place(right[i, :NY_LOCAL], right[12 + i, :NY_LOCAL], g, HALO + 60 + x)
    turn(x_ref, out, 80)


def halos(zb, za, left, right, roots):
    return pl.pallas_call(
        halo_kernel,
        out_shape=jax.ShapeDtypeStruct((80, YPAD, 128), F32),
        in_specs=[pl.BlockSpec(memory_space=VMEM)] * 4 + [pl.BlockSpec(memory_space=SMEM)],
        scratch_shapes=[VMEM((128, NY_LOCAL, 128), F32)],
        compiler_params=vm(20),
        cost_estimate=cost(5),
        name="halos",
    )(zb, za, left, right, roots)


def split_rows(f):
    hi = f.astype(BF16).astype(F32)
    return jnp.concatenate([hi, f - hi], axis=0).astype(BF16)


def both(own, part):
    return split_rows(jnp.concatenate([own, part], axis=0))


def join_mid_kernel(own, part, out):
    def step(z, carry):
        out[HALO + z] = both(own[z], part[z])
        return carry

    lax.fori_loop(0, 128, step, 0, unroll=4)


def join_halo_kernel(full, own, part, out):
    for z in range(HALO):
        out[z] = both(own[z], part[z])
        out[HALO + 128 + z] = both(own[40 + z], part[40 + z])


def join_mid(own, part):
    return pl.pallas_call(
        join_mid_kernel,
        out_shape=jax.ShapeDtypeStruct((128 + 2 * HALO, 4 * YPAD, 128), BF16),
        compiler_params=vm(32),
        cost_estimate=cost(2),
        name="join_mid",
    )(own, part)


def join_halo(full, own, part):
    return pl.pallas_call(
        join_halo_kernel,
        out_shape=jax.ShapeDtypeStruct(full.shape, full.dtype),
        in_specs=[pl.BlockSpec(memory_space=ANY)] + [pl.BlockSpec(memory_space=VMEM)] * 2,
        input_output_aliases={0: 0},
        compiler_params=vm(32),
        cost_estimate=cost(2),
        name="join_halo",
    )(full, own, part)


def placed(table_hi, table_lo, hot):
    hot = jnp.where(hot, 1.0, 0.0).astype(BF16)
    hi = jnp.dot(table_hi, hot, preferred_element_type=F32)
    lo = jnp.dot(table_lo, hot, preferred_element_type=F32)
    top = jnp.concatenate([hi, hi], axis=1)
    low = jnp.concatenate([lo, jnp.zeros_like(lo)], axis=1)
    return jnp.concatenate([top, low], axis=0).astype(BF16)


def folded(r):
    return r[:G] + r[G:]


def locate(roots, place, sizes, slot, holder):
    nx, ny, nz, bx, by, bz = sizes
    ok = jnp.int32(0)
    x0 = y0 = z0 = jnp.int32(0)
    for s in range(slot):
        def rel(dim, origin, total):
            v = roots[holder, dim, s] + HALO - origin
            return jnp.where(v < 0, v + total, jnp.where(v >= total, v - total, v))

        rx = rel(0, place[0] * bx, nx)
        mine = rx < bx
        ok = jnp.where(mine, 1, ok)
        x0 = jnp.where(mine, rx, x0)
        y0 = jnp.where(mine, rel(1, place[1] * by, ny) - HALO, y0)
        z0 = jnp.where(mine, rel(2, place[2] * bz, nz), z0)
    return ok, x0, y0, z0


def field_kernel(shifts, sizes, slot, roots, place, thi, tlo, a2_ref, full, *rest):
    n = len(shifts)
    outs = rest[:n]
    t1, t2, obuf, info, sems = rest[n:]
    gx = place[0]
    py = gx // 4
    px = gx % 4

    for j, (dy, dx) in enumerate(shifts):
        holder = ((py + dy) % 4) * 4 + (px + dx) % 4
        ok, x0, y0, z0 = locate(roots, place, sizes, slot, holder)
        info[0, j] = ok
        info[1, j] = x0
        info[2, j] = y0
        info[3, j] = z0

    def out_copy(k, b):
        return pltpu.make_async_copy(obuf.at[b], outs[k], sems.at[b])

    for b in range(G):
        t1[b * 72 + 64:b * 72 + 72, :] = jnp.zeros((8, 128), F32)

    def compute(j, b):
        x0 = info[1, j]
        y0 = info[2, j]
        z0 = info[3, j]
        k = lax.broadcasted_iota(jnp.int32, (128, 128), 0)
        col = lax.broadcasted_iota(jnp.int32, (128, 128), 1)
        half = col & 63
        near = jnp.where(col < 64, col, col - 4) - y0
        far = jnp.where(col < 64, -1, col - 124 - y0)
        hot_y = jnp.logical_and(half < NY_LOCAL, jnp.logical_or(k == near, k == far))
        a1 = placed(thi[...], tlo[...], hot_y)
        a3 = placed(thi[...], tlo[...], k == col - x0)
        a2 = a2_ref[...]
        for p in range(BOX // 2):
            rhs = jnp.concatenate([full[z0 + 2 * p], full[z0 + 2 * p + 1]], axis=1)
            t = folded(jnp.dot(a1, rhs, preferred_element_type=F32))
            t1[pl.ds(2 * p, G, stride=72), :] = t[:, :128]
            t1[pl.ds(2 * p + 1, G, stride=72), :] = t[:, 128:]
        for q in range(0, G, 2):
            f = jnp.concatenate([t1[q * 72:q * 72 + 72, :], t1[q * 72 + 72:q * 72 + 144, :]], axis=1)
            t = folded(jnp.dot(a2, split_rows(f), preferred_element_type=F32))
            t2[q * G:q * G + G, :] = t[:, :128]
            t2[q * G + G:q * G + 2 * G, :] = t[:, 128:]
        for m in range(9):
            f = t2[256 * m:256 * m + 256, :]
            hi = f.astype(BF16)
            lo = (f - hi.astype(F32)).astype(BF16)
            rhs = jnp.concatenate([hi, lo], axis=1)
            r = lax.dot_general(a3, rhs, (((1,), (1,)), ((), ())), preferred_element_type=F32)
            t = folded(r)
            obuf[b, pl.ds(2 * m, G, stride=18), :] = t[:, :128]
            obuf[b, pl.ds(2 * m + 1, G, stride=18), :] = t[:, 128:]

    def drain(j, b):
        @pl.when(info[0, j] == 1)
        def _():
            out_copy(0, b).wait()

    def step(j, carry):
        b = lax.rem(j, 2)

        @pl.when(j >= 2)
        def _():
            drain(j - 2, b)

        @pl.when(info[0, j] == 1)
        def _():
            compute(j, b)
            for k in range(n):
                @pl.when(j == k)
                def _(k=k):
                    out_copy(k, b).start()

        return carry

    lax.fori_loop(0, n, step, 0)
    drain(n - 2, (n - 2) % 2)
    drain(n - 1, (n - 1) % 2)


def fields(shifts, sizes, slot, roots, place, thi, tlo, a2, full):
    n = len(shifts)
    out = jax.ShapeDtypeStruct((ROWS, 128), F32)
    smem = pl.BlockSpec(memory_space=SMEM)
    vmem = pl.BlockSpec(memory_space=VMEM)
    hbm = pl.BlockSpec(memory_space=ANY)

    def kernel(*refs):
        field_kernel(shifts, sizes, slot, *refs)

    return pl.pallas_call(
        kernel,
        out_shape=(out,) * n,
        in_specs=[smem, smem, vmem, vmem, vmem, vmem],
        out_specs=(hbm,) * n,
        scratch_shapes=[
            VMEM((G * 72, 128), F32),
            VMEM((G * G, 128), F32),
            VMEM((2, ROWS, 128), F32),
            SMEM((4, n), jnp.int32),
            pltpu.SemaphoreType.DMA((2,)),
        ],
        compiler_params=vm(24),
        cost_estimate=cost(FIELD_COST * n),
        name="fields",
    )(roots, place, thi, tlo, a2, full)


def pick_kernel(order, sizes, slot, own_root, place, *rest):
    srcs = rest[:16]
    out, buf, sems = rest[16:]
    nx, bx = sizes[0], sizes[3]
    gx = place[0]
    py = gx // 4
    px = gx % 4
    for s in range(slot):
        r = own_root[0, s] + HALO
        for k, (dy, dx) in enumerate(order):
            anchor = ((py + 4 - dy) % 4) * 4 + (px + 4 - dx) % 4
            v = r - anchor * bx
            v = jnp.where(v < 0, v + nx, jnp.where(v >= nx, v - nx, v))

            @pl.when(v < bx)
            def _(k=k, s=s):
                pltpu.make_async_copy(srcs[k], buf.at[s], sems.at[s]).start()
    for s in range(slot):
        pltpu.make_async_copy(srcs[0], buf.at[s], sems.at[s]).wait()
        out[:, s, :] = buf[s]


def pick(order, sizes, slot, own_root, place, parts):
    smem = pl.BlockSpec(memory_space=SMEM)

    def kernel(*refs):
        pick_kernel(order, sizes, slot, *refs)

    return pl.pallas_call(
        kernel,
        out_shape=jax.ShapeDtypeStruct((ROWS, slot, 128), F32),
        in_specs=[smem, smem] + [pl.BlockSpec(memory_space=ANY)] * 16,
        scratch_shapes=[VMEM((slot, ROWS, 128), F32), pltpu.SemaphoreType.DMA((slot,))],
        compiler_params=vm(8),
        name="pick",
    )(own_root, place, *parts)


def program(potential, frag_root):
    bx, by, bz = potential.shape
    groups = lax.axis_size("gx")
    zs = lax.axis_size("gz")
    sizes = (bx * groups, by * lax.axis_size("gy"), bz * zs, bx, by, bz)
    slot = frag_root.shape[1]
    place = jnp.stack([lax.axis_index("gx"), lax.axis_index("gy"), lax.axis_index("gz")]).astype(jnp.int32)

    def move(v, sx, sz):
        axis, count, by = ("gx", groups, sx) if sx else ("gz", zs, sz)
        return lax.ppermute(v, axis, [(i, (i + by) % count) for i in range(count)])

    before = move(potential[bx - HALO:], 1, 0)
    after = move(potential[:HALO], -1, 0)
    za, zb = pack(potential)
    got_zb = move(zb, 0, 1)
    got_za = move(za, 0, -1)
    left = move(jnp.concatenate([got_zb[8:], got_za[8:]], axis=0), 1, 0)
    right = move(jnp.concatenate([got_zb[:12], got_za[:12]], axis=0), -1, 0)
    roots = lax.all_to_all(
        jnp.broadcast_to(frag_root[None], (groups, 3, slot)), "gx", 0, 0, tiled=True
    )

    swap = [(0, 1), (1, 0)]
    own_m = middle(before, potential, after, zb)
    part_m = lax.ppermute(own_m, "gy", swap)
    full = join_mid(own_m, part_m)
    own_h = halos(got_zb, got_za, left, right, roots)
    part_h = lax.ppermute(own_h, "gy", swap)
    full = join_halo(full, own_h, part_h)

    table = interp_matrix()
    hi = np.asarray(table.astype(BF16))
    lo = (table - hi.astype(np.float32)).astype(BF16)
    thi = np.zeros((G, 128), BF16)
    tlo = np.zeros((G, 128), BF16)
    thi[:, :BOX] = hi
    tlo[:, :BOX] = lo
    a2 = np.zeros((2 * G, 144), BF16)
    a2[:G, :BOX] = hi
    a2[:G, 72:72 + BOX] = hi
    a2[G:, :BOX] = lo

    order = []
    parts = []
    for shifts in GROUPS:
        done = fields(shifts, sizes, slot, roots, place, thi, tlo, a2, full)
        for (dy, dx), v in zip(shifts, done):
            order.append((dy, dx))
            if (dy, dx) != (0, 0):
                perm = [(4 * y + x, 4 * ((y + dy) % 4) + (x + dx) % 4) for y in range(4) for x in range(4)]
                v = lax.ppermute(v, "gx", perm)
            parts.append(v)
    out = pick(tuple(order), sizes, slot, frag_root, place, parts)
    return jnp.transpose(out, (1, 0, 2)).reshape(slot, ROWS * 128)


def solution(mesh):
    return jax.shard_map(
        program,
        mesh=mesh,
        in_specs=(P("gx", "gy", "gz"), P(None, ("gx", "gy", "gz"))),
        out_specs=P(("gx", "gy", "gz"), None),
        check_vma=False,
    )
```

```python
import math

import jax
import jax.numpy as jnp
import numpy as np
from jax import lax
from jax.experimental import pallas as pl
from jax.experimental.pallas import tpu as pltpu
from jax.sharding import PartitionSpec as P


G = 48
BOX = 68
HALO = 34
NY_LOCAL = 60
YPAD = 64
YSTEP = 72
ROWS = G * G * G // 128
F32 = jnp.float32
BF16 = jnp.bfloat16
MID_COST = 10
FIELD_COST = 3
ANY = pl.ANY
VMEM = pltpu.VMEM
SMEM = pltpu.SMEM

GROUPS = (
    ((1, 2), (3, 2)),
    ((2, 1), (2, 3)),
    ((1, 1), (3, 3), (1, 3), (3, 1), (2, 2)),
    ((0, 1), (0, 3), (1, 0), (3, 0), (0, 2), (2, 0), (0, 0)),
)


def interp_matrix():
    a = np.arange(G, dtype=np.float64)[:, None]
    x = np.arange(BOX, dtype=np.float64)[None, :]
    total = np.ones((G, BOX))
    for k in range(1, G // 2):
        total = total + 2.0 * np.cos(2.0 * math.pi * k * (a / G - x / BOX))
    return (total / BOX).astype(np.float32)


def cost(us):
    return pl.CostEstimate(flops=int(us * 1e9), bytes_accessed=0, transcendentals=0)


def vm(limit=48):
    return pltpu.CompilerParams(vmem_limit_bytes=limit << 20)


def pack_rows(p_ref, side, i, lane):
    base, first = (0, 40) if side == 0 else (128 - HALO, 0)
    rows = []
    for g in range(3):
        v = p_ref[3 * i + g]
        shift = (first + HALO * g - base) % 128
        rows.append(pltpu.roll(v, shift, 1) if shift else v)
    at = jnp.where(lane < first, lane + 128 - first, lane - first)
    return jnp.where(at < HALO, rows[0], jnp.where(at < 2 * HALO, rows[1], rows[2]))


def pack_kernel(p_ref, za, zb):
    lane = lax.broadcasted_iota(jnp.int32, (NY_LOCAL, 128), 1)
    for i in range(20):
        za[i, :NY_LOCAL] = pack_rows(p_ref, 0, i, lane)
        zb[i, :NY_LOCAL] = pack_rows(p_ref, 1, i, lane)


def pack(p):
    big = jax.ShapeDtypeStruct((20, YPAD, 128), F32)
    return pl.pallas_call(
        pack_kernel,
        out_shape=(big, big),
        compiler_params=vm(16),
        name="pack",
    )(p)


def turn(src, out, count):
    r = lax.broadcasted_iota(jnp.int32, (count, 256), 0)
    c = lax.broadcasted_iota(jnp.int32, (count, 256), 1) & 127
    pick_z = jnp.where(r == c, 1.0, 0.0).astype(BF16)
    for y in range(0, NY_LOCAL, 2):
        m = jnp.concatenate([src[pl.ds(y + k, 128, stride=YSTEP), :] for k in range(2)], axis=0)
        hi = m.astype(BF16)
        lo = (m - hi.astype(F32)).astype(BF16)
        pair = jnp.concatenate([hi, lo], axis=1)
        t = lax.dot_general(pick_z, pair, (((1,), (1,)), ((), ())), preferred_element_type=F32)
        out[pl.ds(y, count, stride=YSTEP), :] = t[:, :128]
        out[pl.ds(y + 1, count, stride=YSTEP), :] = t[:, 128:]
    for y in range(NY_LOCAL, YPAD):
        out[pl.ds(y, count, stride=YSTEP), :] = jnp.zeros((count, 128), F32)


def mid_kernel(before, own, after, packed, out, x_ref):
    for ref, first, n in ((before, 0, HALO), (own, HALO, 60), (after, HALO + 60, HALO)):
        for i in range(n):
            x_ref[pl.ds(YSTEP * (first + i), NY_LOCAL), :] = ref[i]
    turn(x_ref, out, 128)


def middle(before, own, after, packed):
    return pl.pallas_call(
        mid_kernel,
        out_shape=jax.ShapeDtypeStruct((128 * YSTEP, 128), F32),
        in_specs=[pl.BlockSpec(memory_space=VMEM)] * 3 + [pl.BlockSpec(memory_space=ANY)],
        scratch_shapes=[VMEM((128 * YSTEP, 128), F32)],
        compiler_params=vm(20),
        cost_estimate=cost(MID_COST),
        name="middle",
    )(before, own, after, packed).reshape(128, YSTEP, 128)


def halo_kernel(zb, za, left, right, roots, out, x_ref):
    lane = lax.broadcasted_iota(jnp.int32, (NY_LOCAL, 128), 1)

    def place(b, a, g, row):
        mine = jnp.logical_and(lane >= HALO * g, lane < HALO * g + HALO)
        v = jnp.where(mine, b, a)
        x_ref[pl.ds(YSTEP * row, NY_LOCAL), :] = pltpu.roll(v, 128 - HALO * g, 1) if g else v

    for g in range(3):
        for i in range(20):
            place(zb[i, :NY_LOCAL], za[i, :NY_LOCAL], g, HALO + 3 * i + g)
        for i in range(12):
            x = 3 * i + g - 2
            if x >= 0:
                place(left[i, :NY_LOCAL], left[12 + i, :NY_LOCAL], g, x)
            x = 3 * i + g
            if x < HALO:
                place(right[i, :NY_LOCAL], right[12 + i, :NY_LOCAL], g, HALO + 60 + x)
    turn(x_ref, out, 80)


def halos(zb, za, left, right, roots):
    return pl.pallas_call(
        halo_kernel,
        out_shape=jax.ShapeDtypeStruct((80 * YSTEP, 128), F32),
        in_specs=[pl.BlockSpec(memory_space=VMEM)] * 4 + [pl.BlockSpec(memory_space=SMEM)],
        scratch_shapes=[VMEM((128 * YSTEP, 128), F32)],
        compiler_params=vm(20),
        cost_estimate=cost(5),
        name="halos",
    )(zb, za, left, right, roots).reshape(80, YSTEP, 128)


def split_rows(f):
    hi = f.astype(BF16).astype(F32)
    return jnp.concatenate([hi, f - hi], axis=0).astype(BF16)


def both(own, part):
    return split_rows(jnp.concatenate([own, part], axis=0))


def join_mid_kernel(own, part, out):
    def step(z, carry):
        out[HALO + z] = both(own[z, :YPAD], part[z, :YPAD])
        return carry

    lax.fori_loop(0, 128, step, 0, unroll=4)


def join_halo_kernel(full, own, part, out):
    for z in range(HALO):
        out[z] = both(own[z, :YPAD], part[z, :YPAD])
        out[HALO + 128 + z] = both(own[40 + z, :YPAD], part[40 + z, :YPAD])


def join_mid(own, part):
    return pl.pallas_call(
        join_mid_kernel,
        out_shape=jax.ShapeDtypeStruct((128 + 2 * HALO, 4 * YPAD, 128), BF16),
        compiler_params=vm(32),
        cost_estimate=cost(2),
        name="join_mid",
    )(own, part)


def join_halo(full, own, part):
    return pl.pallas_call(
        join_halo_kernel,
        out_shape=jax.ShapeDtypeStruct(full.shape, full.dtype),
        in_specs=[pl.BlockSpec(memory_space=ANY)] + [pl.BlockSpec(memory_space=VMEM)] * 2,
        input_output_aliases={0: 0},
        compiler_params=vm(32),
        cost_estimate=cost(2),
        name="join_halo",
    )(full, own, part)


def placed(table_hi, table_lo, hot):
    hot = jnp.where(hot, 1.0, 0.0).astype(BF16)
    hi = jnp.dot(table_hi, hot, preferred_element_type=F32)
    lo = jnp.dot(table_lo, hot, preferred_element_type=F32)
    top = jnp.concatenate([hi, hi], axis=1)
    low = jnp.concatenate([lo, jnp.zeros_like(lo)], axis=1)
    return jnp.concatenate([top, low], axis=0).astype(BF16)


def folded(r):
    return r[:G] + r[G:]


def locate(roots, place, sizes, slot, holder):
    nx, ny, nz, bx, by, bz = sizes
    ok = jnp.int32(0)
    x0 = y0 = z0 = jnp.int32(0)
    for s in range(slot):
        def rel(dim, origin, total):
            v = roots[holder, dim, s] + HALO - origin
            return jnp.where(v < 0, v + total, jnp.where(v >= total, v - total, v))

        rx = rel(0, place[0] * bx, nx)
        mine = rx < bx
        ok = jnp.where(mine, 1, ok)
        x0 = jnp.where(mine, rx, x0)
        y0 = jnp.where(mine, rel(1, place[1] * by, ny) - HALO, y0)
        z0 = jnp.where(mine, rel(2, place[2] * bz, nz), z0)
    return ok, x0, y0, z0


def field_kernel(shifts, sizes, slot, roots, place, thi, tlo, a2_ref, full, *rest):
    n = len(shifts)
    outs = rest[:n]
    t1, t2, obuf, info, sems = rest[n:]
    gx = place[0]
    py = gx // 4
    px = gx % 4

    for j, (dy, dx) in enumerate(shifts):
        holder = ((py + dy) % 4) * 4 + (px + dx) % 4
        ok, x0, y0, z0 = locate(roots, place, sizes, slot, holder)
        info[0, j] = ok
        info[1, j] = x0
        info[2, j] = y0
        info[3, j] = z0

    def out_copy(k, b):
        return pltpu.make_async_copy(obuf.at[b], outs[k], sems.at[b])

    for b in range(G):
        t1[b * 72 + 64:b * 72 + 72, :] = jnp.zeros((8, 128), F32)

    def compute(j, b):
        x0 = info[1, j]
        y0 = info[2, j]
        z0 = info[3, j]
        k = lax.broadcasted_iota(jnp.int32, (128, 128), 0)
        col = lax.broadcasted_iota(jnp.int32, (128, 128), 1)
        half = col & 63
        near = jnp.where(col < 64, col, col - 4) - y0
        far = jnp.where(col < 64, -1, col - 124 - y0)
        hot_y = jnp.logical_and(half < NY_LOCAL, jnp.logical_or(k == near, k == far))
        a1 = placed(thi[...], tlo[...], hot_y)
        a3 = placed(thi[...], tlo[...], k == col - x0)
        a2 = a2_ref[...]
        for p in range(BOX // 2):
            rhs = jnp.concatenate([full[z0 + 2 * p], full[z0 + 2 * p + 1]], axis=1)
            t = folded(jnp.dot(a1, rhs, preferred_element_type=F32))
            t1[pl.ds(2 * p, G, stride=72), :] = t[:, :128]
            t1[pl.ds(2 * p + 1, G, stride=72), :] = t[:, 128:]
        for q in range(0, G, 2):
            f = jnp.concatenate([t1[q * 72:q * 72 + 72, :], t1[q * 72 + 72:q * 72 + 144, :]], axis=1)
            t = folded(jnp.dot(a2, split_rows(f), preferred_element_type=F32))
            t2[q * G:q * G + G, :] = t[:, :128]
            t2[q * G + G:q * G + 2 * G, :] = t[:, 128:]
        for m in range(9):
            f = t2[256 * m:256 * m + 256, :]
            hi = f.astype(BF16)
            lo = (f - hi.astype(F32)).astype(BF16)
            rhs = jnp.concatenate([hi, lo], axis=1)
            r = lax.dot_general(a3, rhs, (((1,), (1,)), ((), ())), preferred_element_type=F32)
            t = folded(r)
            obuf[b, pl.ds(2 * m, G, stride=18), :] = t[:, :128]
            obuf[b, pl.ds(2 * m + 1, G, stride=18), :] = t[:, 128:]

    def drain(j, b):
        @pl.when(info[0, j] == 1)
        def _():
            out_copy(0, b).wait()

    def step(j, carry):
        b = lax.rem(j, 2)

        @pl.when(j >= 2)
        def _():
            drain(j - 2, b)

        @pl.when(info[0, j] == 1)
        def _():
            compute(j, b)
            for k in range(n):
                @pl.when(j == k)
                def _(k=k):
                    out_copy(k, b).start()

        return carry

    lax.fori_loop(0, n, step, 0)
    drain(n - 2, (n - 2) % 2)
    drain(n - 1, (n - 1) % 2)


def fields(shifts, sizes, slot, roots, place, thi, tlo, a2, full):
    n = len(shifts)
    out = jax.ShapeDtypeStruct((ROWS, 128), F32)
    smem = pl.BlockSpec(memory_space=SMEM)
    vmem = pl.BlockSpec(memory_space=VMEM)
    hbm = pl.BlockSpec(memory_space=ANY)

    def kernel(*refs):
        field_kernel(shifts, sizes, slot, *refs)

    return pl.pallas_call(
        kernel,
        out_shape=(out,) * n,
        in_specs=[smem, smem, vmem, vmem, vmem, vmem],
        out_specs=(hbm,) * n,
        scratch_shapes=[
            VMEM((G * 72, 128), F32),
            VMEM((G * G, 128), F32),
            VMEM((2, ROWS, 128), F32),
            SMEM((4, n), jnp.int32),
            pltpu.SemaphoreType.DMA((2,)),
        ],
        compiler_params=vm(24),
        cost_estimate=cost(FIELD_COST * n),
        name="fields",
    )(roots, place, thi, tlo, a2, full)


def pick_kernel(order, sizes, slot, own_root, place, *rest):
    srcs = rest[:16]
    out, buf, sems = rest[16:]
    nx, bx = sizes[0], sizes[3]
    gx = place[0]
    py = gx // 4
    px = gx % 4
    for s in range(slot):
        r = own_root[0, s] + HALO
        for k, (dy, dx) in enumerate(order):
            anchor = ((py + 4 - dy) % 4) * 4 + (px + 4 - dx) % 4
            v = r - anchor * bx
            v = jnp.where(v < 0, v + nx, jnp.where(v >= nx, v - nx, v))

            @pl.when(v < bx)
            def _(k=k, s=s):
                pltpu.make_async_copy(srcs[k], buf.at[s], sems.at[s]).start()
    for s in range(slot):
        pltpu.make_async_copy(srcs[0], buf.at[s], sems.at[s]).wait()
        out[pl.ds(s, ROWS, stride=slot), :] = buf[s]


def pick(order, sizes, slot, own_root, place, parts):
    smem = pl.BlockSpec(memory_space=SMEM)

    def kernel(*refs):
        pick_kernel(order, sizes, slot, *refs)

    return pl.pallas_call(
        kernel,
        out_shape=jax.ShapeDtypeStruct((ROWS * slot, 128), F32),
        in_specs=[smem, smem] + [pl.BlockSpec(memory_space=ANY)] * 16,
        scratch_shapes=[VMEM((slot, ROWS, 128), F32), pltpu.SemaphoreType.DMA((slot,))],
        compiler_params=vm(8),
        name="pick",
    )(own_root, place, *parts)


def program(potential, frag_root):
    bx, by, bz = potential.shape
    groups = lax.axis_size("gx")
    zs = lax.axis_size("gz")
    sizes = (bx * groups, by * lax.axis_size("gy"), bz * zs, bx, by, bz)
    slot = frag_root.shape[1]
    place = jnp.stack([lax.axis_index("gx"), lax.axis_index("gy"), lax.axis_index("gz")]).astype(jnp.int32)

    def move(v, sx, sz):
        axis, count, by = ("gx", groups, sx) if sx else ("gz", zs, sz)
        return lax.ppermute(v, axis, [(i, (i + by) % count) for i in range(count)])

    before = move(potential[bx - HALO:], 1, 0)
    after = move(potential[:HALO], -1, 0)
    za, zb = pack(potential)
    got_zb = move(zb, 0, 1)
    got_za = move(za, 0, -1)
    left = move(jnp.concatenate([got_zb[8:], got_za[8:]], axis=0), 1, 0)
    right = move(jnp.concatenate([got_zb[:12], got_za[:12]], axis=0), -1, 0)
    roots = lax.all_to_all(
        jnp.broadcast_to(frag_root[None], (groups, 3, slot)), "gx", 0, 0, tiled=True
    )

    swap = [(0, 1), (1, 0)]
    own_m = middle(before, potential, after, zb)
    part_m = lax.ppermute(own_m, "gy", swap)
    full = join_mid(own_m, part_m)
    own_h = halos(got_zb, got_za, left, right, roots)
    part_h = lax.ppermute(own_h, "gy", swap)
    full = join_halo(full, own_h, part_h)

    table = interp_matrix()
    hi = np.asarray(table.astype(BF16))
    lo = (table - hi.astype(np.float32)).astype(BF16)
    thi = np.zeros((G, 128), BF16)
    tlo = np.zeros((G, 128), BF16)
    thi[:, :BOX] = hi
    tlo[:, :BOX] = lo
    a2 = np.zeros((2 * G, 144), BF16)
    a2[:G, :BOX] = hi
    a2[:G, 72:72 + BOX] = hi
    a2[G:, :BOX] = lo

    order = []
    parts = []
    for shifts in GROUPS:
        done = fields(shifts, sizes, slot, roots, place, thi, tlo, a2, full)
        for (dy, dx), v in zip(shifts, done):
            order.append((dy, dx))
            if (dy, dx) != (0, 0):
                perm = [(4 * y + x, 4 * ((y + dy) % 4) + (x + dx) % 4) for y in range(4) for x in range(4)]
                v = lax.ppermute(v, "gx", perm)
            parts.append(v)
    out = pick(tuple(order), sizes, slot, frag_root, place, parts)
    return jnp.transpose(out.reshape(ROWS, slot, 128), (1, 0, 2)).reshape(slot, ROWS * 128)


def solution(mesh):
    return jax.shard_map(
        program,
        mesh=mesh,
        in_specs=(P("gx", "gy", "gz"), P(None, ("gx", "gy", "gz"))),
        out_specs=P(("gx", "gy", "gz"), None),
        check_vma=False,
    )
```

```python
import math

import jax
import jax.numpy as jnp
import numpy as np
from jax import lax
from jax.experimental import pallas as pl
from jax.experimental.pallas import tpu as pltpu
from jax.sharding import PartitionSpec as P


G = 48
BOX = 68
HALO = 34
NY_LOCAL = 60
YPAD = 64
YSTEP = 72
ROWS = G * G * G // 128
F32 = jnp.float32
BF16 = jnp.bfloat16
MID_COST = 10
FIELD_COST = 3
ANY = pl.ANY
VMEM = pltpu.VMEM
SMEM = pltpu.SMEM


def interp_matrix():
    a = np.arange(G, dtype=np.float64)[:, None]
    x = np.arange(BOX, dtype=np.float64)[None, :]
    total = np.ones((G, BOX))
    for k in range(1, G // 2):
        total = total + 2.0 * np.cos(2.0 * math.pi * k * (a / G - x / BOX))
    return (total / BOX).astype(np.float32)


def cost(us):
    return pl.CostEstimate(flops=int(us * 1e9), bytes_accessed=0, transcendentals=0)


def vm(limit=48):
    return pltpu.CompilerParams(vmem_limit_bytes=limit << 20)


def pack_rows(p_ref, side, i, lane):
    base, first = (0, 40) if side == 0 else (128 - HALO, 0)
    rows = []
    for g in range(3):
        v = p_ref[3 * i + g]
        shift = (first + HALO * g - base) % 128
        rows.append(pltpu.roll(v, shift, 1) if shift else v)
    at = jnp.where(lane < first, lane + 128 - first, lane - first)
    return jnp.where(at < HALO, rows[0], jnp.where(at < 2 * HALO, rows[1], rows[2]))


def pack_kernel(p_ref, za, zb):
    lane = lax.broadcasted_iota(jnp.int32, (NY_LOCAL, 128), 1)
    for i in range(20):
        za[i, :NY_LOCAL] = pack_rows(p_ref, 0, i, lane)
        zb[i, :NY_LOCAL] = pack_rows(p_ref, 1, i, lane)


def pack(p):
    big = jax.ShapeDtypeStruct((20, YPAD, 128), F32)
    return pl.pallas_call(
        pack_kernel,
        out_shape=(big, big),
        compiler_params=vm(10),
        name="pack",
    )(p)


def turn(src, out, count):
    r = lax.broadcasted_iota(jnp.int32, (count, 256), 0)
    c = lax.broadcasted_iota(jnp.int32, (count, 256), 1) & 127
    pick_z = jnp.where(r == c, 1.0, 0.0).astype(BF16)
    for y in range(0, NY_LOCAL, 2):
        m = jnp.concatenate([src[pl.ds(y + k, 128, stride=YSTEP), :] for k in range(2)], axis=0)
        hi = m.astype(BF16)
        lo = (m - hi.astype(F32)).astype(BF16)
        pair = jnp.concatenate([hi, lo], axis=1)
        t = lax.dot_general(pick_z, pair, (((1,), (1,)), ((), ())), preferred_element_type=F32)
        out[pl.ds(y, count, stride=YSTEP), :] = t[:, :128]
        out[pl.ds(y + 1, count, stride=YSTEP), :] = t[:, 128:]
    for y in range(NY_LOCAL, YPAD):
        out[pl.ds(y, count, stride=YSTEP), :] = jnp.zeros((count, 128), F32)


def mid_kernel(before, own, after, packed, out, x_ref):
    for ref, first, n in ((before, 0, HALO), (own, HALO, 60), (after, HALO + 60, HALO)):
        for i in range(n):
            x_ref[pl.ds(YSTEP * (first + i), NY_LOCAL), :] = ref[i]
    turn(x_ref, out, 128)


def middle(before, own, after, packed):
    return pl.pallas_call(
        mid_kernel,
        out_shape=jax.ShapeDtypeStruct((128 * YSTEP, 128), F32),
        in_specs=[pl.BlockSpec(memory_space=VMEM)] * 3 + [pl.BlockSpec(memory_space=ANY)],
        scratch_shapes=[VMEM((128 * YSTEP, 128), F32)],
        compiler_params=vm(18),
        cost_estimate=cost(MID_COST),
        name="middle",
    )(before, own, after, packed).reshape(128, YSTEP, 128)


def halo_kernel(zb, za, left, right, roots, out, x_ref):
    lane = lax.broadcasted_iota(jnp.int32, (NY_LOCAL, 128), 1)

    def place(b, a, g, row):
        mine = jnp.logical_and(lane >= HALO * g, lane < HALO * g + HALO)
        v = jnp.where(mine, b, a)
        x_ref[pl.ds(YSTEP * row, NY_LOCAL), :] = pltpu.roll(v, 128 - HALO * g, 1) if g else v

    for g in range(3):
        for i in range(20):
            place(zb[i, :NY_LOCAL], za[i, :NY_LOCAL], g, HALO + 3 * i + g)
        for i in range(12):
            x = 3 * i + g - 2
            if x >= 0:
                place(left[i, :NY_LOCAL], left[12 + i, :NY_LOCAL], g, x)
            x = 3 * i + g
            if x < HALO:
                place(right[i, :NY_LOCAL], right[12 + i, :NY_LOCAL], g, HALO + 60 + x)
    turn(x_ref, out, 80)


def halos(zb, za, left, right, roots):
    return pl.pallas_call(
        halo_kernel,
        out_shape=jax.ShapeDtypeStruct((80 * YSTEP, 128), F32),
        in_specs=[pl.BlockSpec(memory_space=VMEM)] * 4 + [pl.BlockSpec(memory_space=SMEM)],
        scratch_shapes=[VMEM((128 * YSTEP, 128), F32)],
        compiler_params=vm(16),
        cost_estimate=cost(5),
        name="halos",
    )(zb, za, left, right, roots).reshape(80, YSTEP, 128)


def split_rows(f):
    hi = f.astype(BF16).astype(F32)
    return jnp.concatenate([hi, f - hi], axis=0).astype(BF16)


def both(own, part):
    return split_rows(jnp.concatenate([own, part], axis=0))


CHUNK = 16


def join_mid_kernel(own, part, out, own_v, part_v, sems):
    def copies(n):
        rows = pl.ds(n * CHUNK, CHUNK)
        return (
            pltpu.make_async_copy(own.at[rows], own_v.at[rows], sems.at[0, n]),
            pltpu.make_async_copy(part.at[rows], part_v.at[rows], sems.at[1, n]),
        )

    for n in range(128 // CHUNK):
        for c in copies(n):
            c.start()
    for n in range(128 // CHUNK):
        for c in copies(n):
            c.wait()

        def step(i, carry):
            z = n * CHUNK + i
            out[HALO + z] = both(own_v[z, :YPAD], part_v[z, :YPAD])
            return carry

        lax.fori_loop(0, CHUNK, step, 0, unroll=4)


def join_halo_kernel(full, own, part, out):
    for z in range(HALO):
        out[z] = both(own[z, :YPAD], part[z, :YPAD])
        out[HALO + 128 + z] = both(own[40 + z, :YPAD], part[40 + z, :YPAD])


def join_mid(own, part):
    return pl.pallas_call(
        join_mid_kernel,
        out_shape=jax.ShapeDtypeStruct((128 + 2 * HALO, 4 * YPAD, 128), BF16),
        in_specs=[pl.BlockSpec(memory_space=ANY)] * 2,
        scratch_shapes=[
            VMEM((128, YSTEP, 128), F32),
            VMEM((128, YSTEP, 128), F32),
            pltpu.SemaphoreType.DMA((2, 128 // CHUNK)),
        ],
        compiler_params=vm(14),
        cost_estimate=cost(2),
        name="join_mid",
    )(own, part)


def join_halo(full, own, part):
    return pl.pallas_call(
        join_halo_kernel,
        out_shape=jax.ShapeDtypeStruct(full.shape, full.dtype),
        in_specs=[
            pl.BlockSpec(memory_space=ANY),
            pl.BlockSpec(memory_space=VMEM),
            pl.BlockSpec(memory_space=VMEM),
        ],
        input_output_aliases={0: 0},
        compiler_params=vm(10),
        cost_estimate=cost(2),
        name="join_halo",
    )(full, own, part)


def placed(table_hi, table_lo, hot):
    hot = jnp.where(hot, 1.0, 0.0).astype(BF16)
    hi = jnp.dot(table_hi, hot, preferred_element_type=F32)
    lo = jnp.dot(table_lo, hot, preferred_element_type=F32)
    top = jnp.concatenate([hi, hi], axis=1)
    low = jnp.concatenate([lo, jnp.zeros_like(lo)], axis=1)
    return jnp.concatenate([top, low], axis=0).astype(BF16)


def folded(r):
    return r[:G] + r[G:]


def locate(roots, place, sizes, slot, holder):
    nx, ny, nz, bx, by, bz = sizes
    ok = jnp.int32(0)
    x0 = y0 = z0 = jnp.int32(0)
    for s in range(slot):
        def rel(dim, origin, total):
            v = roots[holder, dim, s] + HALO - origin
            return jnp.where(v < 0, v + total, jnp.where(v >= total, v - total, v))

        rx = rel(0, place[0] * bx, nx)
        mine = rx < bx
        ok = jnp.where(mine, 1, ok)
        x0 = jnp.where(mine, rx, x0)
        y0 = jnp.where(mine, rel(1, place[1] * by, ny) - HALO, y0)
        z0 = jnp.where(mine, rel(2, place[2] * bz, nz), z0)
    return ok, x0, y0, z0


def field_kernel(late, sizes, slot, n, roots, place, thi, tlo, a2_ref, full, out, t1, t2, obuf, info, sems):
    def find(j, carry):
        ok, x0, y0, z0 = locate(roots, place, sizes, slot, j)
        inside = jnp.logical_and(z0 >= HALO, z0 <= HALO + 128 - BOX)
        info[0, j] = jnp.where(inside, 0, ok) if late else jnp.where(inside, ok, 0)
        info[1, j] = x0
        info[2, j] = y0
        info[3, j] = z0
        return carry

    lax.fori_loop(0, n, find, 0)

    def out_copy(j, b):
        return pltpu.make_async_copy(obuf.at[b], out.at[j], sems.at[b])

    for b in range(G):
        t1[b * 72 + 64:b * 72 + 72, :] = jnp.zeros((8, 128), F32)

    def compute(j, b):
        x0 = info[1, j]
        y0 = info[2, j]
        z0 = info[3, j]
        k = lax.broadcasted_iota(jnp.int32, (128, 128), 0)
        col = lax.broadcasted_iota(jnp.int32, (128, 128), 1)
        half = col & 63
        near = jnp.where(col < 64, col, col - 4) - y0
        far = jnp.where(col < 64, -1, col - 124 - y0)
        hot_y = jnp.logical_and(half < NY_LOCAL, jnp.logical_or(k == near, k == far))
        a1 = placed(thi[...], tlo[...], hot_y)
        a3 = placed(thi[...], tlo[...], k == col - x0)
        a2 = a2_ref[...]
        for p in range(BOX // 2):
            rhs = jnp.concatenate([full[z0 + 2 * p], full[z0 + 2 * p + 1]], axis=1)
            t = folded(jnp.dot(a1, rhs, preferred_element_type=F32))
            t1[pl.ds(2 * p, G, stride=72), :] = t[:, :128]
            t1[pl.ds(2 * p + 1, G, stride=72), :] = t[:, 128:]
        for q in range(0, G, 2):
            f = jnp.concatenate([t1[q * 72:q * 72 + 72, :], t1[q * 72 + 72:q * 72 + 144, :]], axis=1)
            t = folded(jnp.dot(a2, split_rows(f), preferred_element_type=F32))
            t2[q * G:q * G + G, :] = t[:, :128]
            t2[q * G + G:q * G + 2 * G, :] = t[:, 128:]
        for m in range(9):
            f = t2[256 * m:256 * m + 256, :]
            hi = f.astype(BF16)
            lo = (f - hi.astype(F32)).astype(BF16)
            rhs = jnp.concatenate([hi, lo], axis=1)
            r = lax.dot_general(a3, rhs, (((1,), (1,)), ((), ())), preferred_element_type=F32)
            t = folded(r)
            obuf[b, pl.ds(2 * m, G, stride=18), :] = t[:, :128]
            obuf[b, pl.ds(2 * m + 1, G, stride=18), :] = t[:, 128:]

    def drain(j, b):
        @pl.when(info[0, j] == 1)
        def _():
            out_copy(0, b).wait()

    def step(j, carry):
        b = lax.rem(j, 2)

        @pl.when(j >= 2)
        def _():
            drain(j - 2, b)

        @pl.when(info[0, j] == 1)
        def _():
            compute(j, b)
            out_copy(j, b).start()

        return carry

    lax.fori_loop(0, n, step, 0)
    drain(n - 2, (n - 2) % 2)
    drain(n - 1, (n - 1) % 2)


def fields(sizes, slot, n, roots, place, thi, tlo, a2, full, done=None):
    smem = pl.BlockSpec(memory_space=SMEM)
    vmem = pl.BlockSpec(memory_space=VMEM)
    hbm = pl.BlockSpec(memory_space=ANY)
    late = done is not None
    out = jax.ShapeDtypeStruct((n, ROWS, 128), F32)

    def kernel(*refs):
        if late:
            field_kernel(True, sizes, slot, n, *refs[:6], *refs[7:])
        else:
            field_kernel(False, sizes, slot, n, *refs[:7], *refs[8:])

    args = (roots, place, thi, tlo, a2, full) + ((done,) if late else ())
    return pl.pallas_call(
        kernel,
        out_shape=(out,) if late else (out, jax.ShapeDtypeStruct(full.shape, full.dtype)),
        in_specs=[smem, smem, vmem, vmem, vmem, vmem] + [hbm] * late,
        out_specs=(hbm,) if late else (hbm, hbm),
        scratch_shapes=[
            VMEM((G * 72, 128), F32),
            VMEM((G * G, 128), F32),
            VMEM((2, ROWS, 128), F32),
            SMEM((4, n), jnp.int32),
            pltpu.SemaphoreType.DMA((2,)),
        ],
        input_output_aliases={6: 0} if late else {5: 1},
        compiler_params=vm(8),
        cost_estimate=cost(FIELD_COST * n),
        name="fields",
    )(*args)


def pick_kernel(sizes, slot, n, own_root, parts, out, buf, sems):
    nx, bx = sizes[0], sizes[3]
    for s in range(slot):
        r = own_root[0, s] + HALO
        r = jnp.where(r >= nx, r - nx, r)

        def scan(j, anchor):
            return jnp.where(r >= j * bx, j, anchor)

        anchor = lax.fori_loop(0, n, scan, jnp.int32(0), unroll=True)
        pltpu.make_async_copy(parts.at[anchor], buf.at[s], sems.at[s]).start()
    for s in range(slot):
        pltpu.make_async_copy(parts.at[0], buf.at[s], sems.at[s]).wait()
        out[pl.ds(s, ROWS, stride=slot), :] = buf[s]


def pick(sizes, slot, n, own_root, parts):
    def kernel(*refs):
        pick_kernel(sizes, slot, n, *refs)

    return pl.pallas_call(
        kernel,
        out_shape=jax.ShapeDtypeStruct((ROWS * slot, 128), F32),
        in_specs=[pl.BlockSpec(memory_space=SMEM), pl.BlockSpec(memory_space=ANY)],
        scratch_shapes=[VMEM((slot, ROWS, 128), F32), pltpu.SemaphoreType.DMA((slot,))],
        compiler_params=vm(8),
        name="pick",
    )(own_root, parts)


def program(potential, frag_root):
    bx, by, bz = potential.shape
    groups = lax.axis_size("gx")
    zs = lax.axis_size("gz")
    sizes = (bx * groups, by * lax.axis_size("gy"), bz * zs, bx, by, bz)
    slot = frag_root.shape[1]
    place = jnp.stack([lax.axis_index("gx"), lax.axis_index("gy"), lax.axis_index("gz")]).astype(jnp.int32)

    def move(v, sx, sz):
        axis, count, by = ("gx", groups, sx) if sx else ("gz", zs, sz)
        return lax.ppermute(v, axis, [(i, (i + by) % count) for i in range(count)])

    before = move(potential[bx - HALO:], 1, 0)
    after = move(potential[:HALO], -1, 0)
    za, zb = pack(potential)
    got_zb = move(zb, 0, 1)
    got_za = move(za, 0, -1)
    left = move(jnp.concatenate([got_zb[8:], got_za[8:]], axis=0), 1, 0)
    right = move(jnp.concatenate([got_zb[:12], got_za[:12]], axis=0), -1, 0)
    roots = lax.all_to_all(
        jnp.broadcast_to(frag_root[None], (groups, 3, slot)), "gx", 0, 0, tiled=True
    )

    swap = [(0, 1), (1, 0)]
    own_m = middle(before, potential, after, zb)
    part_m = lax.ppermute(own_m, "gy", swap)
    full = join_mid(own_m, part_m)
    own_h = halos(got_zb, got_za, left, right, roots)
    part_h = lax.ppermute(own_h, "gy", swap)

    table = interp_matrix()
    hi = np.asarray(table.astype(BF16))
    lo = (table - hi.astype(np.float32)).astype(BF16)
    thi = np.zeros((G, 128), BF16)
    tlo = np.zeros((G, 128), BF16)
    thi[:, :BOX] = hi
    tlo[:, :BOX] = lo
    a2 = np.zeros((2 * G, 144), BF16)
    a2[:G, :BOX] = hi
    a2[:G, 72:72 + BOX] = hi
    a2[G:, :BOX] = lo

    done, full = fields(sizes, slot, groups, roots, place, thi, tlo, a2, full)
    full = join_halo(full, own_h, part_h)
    (done,) = fields(sizes, slot, groups, roots, place, thi, tlo, a2, full, done)
    parts = lax.all_to_all(done, "gx", 0, 0, tiled=True)
    out = pick(sizes, slot, groups, frag_root, parts)
    return jnp.transpose(out.reshape(ROWS, slot, 128), (1, 0, 2)).reshape(slot, ROWS * 128)


def solution(mesh):
    return jax.shard_map(
        program,
        mesh=mesh,
        in_specs=(P("gx", "gy", "gz"), P(None, ("gx", "gy", "gz"))),
        out_specs=P(("gx", "gy", "gz"), None),
        check_vma=False,
    )
```

```python
import math

import jax
import jax.numpy as jnp
import numpy as np
from jax import lax
from jax.experimental import pallas as pl
from jax.experimental.pallas import tpu as pltpu
from jax.sharding import PartitionSpec as P


G = 48
BOX = 68
HALO = 34
NY_LOCAL = 60
YPAD = 64
YSTEP = 72
ROWS = G * G * G // 128
F32 = jnp.float32
BF16 = jnp.bfloat16
MID_COST = 10
FIELD_COST = 3
ANY = pl.ANY
VMEM = pltpu.VMEM
SMEM = pltpu.SMEM


def interp_matrix():
    a = np.arange(G, dtype=np.float64)[:, None]
    x = np.arange(BOX, dtype=np.float64)[None, :]
    total = np.ones((G, BOX))
    for k in range(1, G // 2):
        total = total + 2.0 * np.cos(2.0 * math.pi * k * (a / G - x / BOX))
    return (total / BOX).astype(np.float32)


def cost(us):
    return pl.CostEstimate(flops=int(us * 1e9), bytes_accessed=0, transcendentals=0)


def vm(limit=48):
    return pltpu.CompilerParams(vmem_limit_bytes=limit << 20)


def pack_rows(p_ref, side, i, lane):
    base, first = (0, 40) if side == 0 else (128 - HALO, 0)
    rows = []
    for g in range(3):
        v = p_ref[3 * i + g]
        shift = (first + HALO * g - base) % 128
        rows.append(pltpu.roll(v, shift, 1) if shift else v)
    at = jnp.where(lane < first, lane + 128 - first, lane - first)
    return jnp.where(at < HALO, rows[0], jnp.where(at < 2 * HALO, rows[1], rows[2]))


def pack_kernel(p_ref, za, zb):
    lane = lax.broadcasted_iota(jnp.int32, (NY_LOCAL, 128), 1)
    for i in range(20):
        za[i, :NY_LOCAL] = pack_rows(p_ref, 0, i, lane)
        zb[i, :NY_LOCAL] = pack_rows(p_ref, 1, i, lane)


def pack(p):
    big = jax.ShapeDtypeStruct((20, YPAD, 128), F32)
    return pl.pallas_call(
        pack_kernel,
        out_shape=(big, big),
        compiler_params=vm(10),
        name="pack",
    )(p)


def turn(src, out, count):
    r = lax.broadcasted_iota(jnp.int32, (count, 256), 0)
    c = lax.broadcasted_iota(jnp.int32, (count, 256), 1) & 127
    pick_z = jnp.where(r == c, 1.0, 0.0).astype(BF16)
    for y in range(0, NY_LOCAL, 2):
        m = jnp.concatenate([src[pl.ds(y + k, 128, stride=YSTEP), :] for k in range(2)], axis=0)
        hi = m.astype(BF16)
        lo = (m - hi.astype(F32)).astype(BF16)
        pair = jnp.concatenate([hi, lo], axis=1)
        t = lax.dot_general(pick_z, pair, (((1,), (1,)), ((), ())), preferred_element_type=F32)
        out[pl.ds(y, count, stride=YSTEP), :] = t[:, :128]
        out[pl.ds(y + 1, count, stride=YSTEP), :] = t[:, 128:]
    for y in range(NY_LOCAL, YPAD):
        out[pl.ds(y, count, stride=YSTEP), :] = jnp.zeros((count, 128), F32)


def mid_kernel(before, own, after, part_before, part_own, part_after, packed, out, x_ref, t_own, t_part):
    for refs, turned in (((before, own, after), t_own), ((part_before, part_own, part_after), t_part)):
        for ref, first, n in zip(refs, (0, HALO, HALO + 60), (HALO, 60, HALO)):
            for i in range(n):
                x_ref[pl.ds(YSTEP * (first + i), NY_LOCAL), :] = ref[i]
        turn(x_ref, turned, 128)

    def step(z, carry):
        rows = pl.ds(pl.multiple_of(z * YSTEP, 8), YPAD)
        out[HALO + z] = both(t_own[rows, :], t_part[rows, :])
        return carry

    lax.fori_loop(0, 128, step, 0, unroll=4)


def middle(before, own, after, part_before, part_own, part_after, packed):
    return pl.pallas_call(
        mid_kernel,
        out_shape=jax.ShapeDtypeStruct((128 + 2 * HALO, 4 * YPAD, 128), BF16),
        in_specs=[pl.BlockSpec(memory_space=VMEM)] * 6 + [pl.BlockSpec(memory_space=ANY)],
        scratch_shapes=[VMEM((128 * YSTEP, 128), F32)] * 3,
        compiler_params=vm(40),
        cost_estimate=cost(MID_COST),
        name="middle",
    )(before, own, after, part_before, part_own, part_after, packed)


def halo_kernel(zb, za, left, right, roots, out, x_ref):
    lane = lax.broadcasted_iota(jnp.int32, (NY_LOCAL, 128), 1)

    def place(b, a, g, row):
        mine = jnp.logical_and(lane >= HALO * g, lane < HALO * g + HALO)
        v = jnp.where(mine, b, a)
        x_ref[pl.ds(YSTEP * row, NY_LOCAL), :] = pltpu.roll(v, 128 - HALO * g, 1) if g else v

    for g in range(3):
        for i in range(20):
            place(zb[i, :NY_LOCAL], za[i, :NY_LOCAL], g, HALO + 3 * i + g)
        for i in range(12):
            x = 3 * i + g - 2
            if x >= 0:
                place(left[i, :NY_LOCAL], left[12 + i, :NY_LOCAL], g, x)
            x = 3 * i + g
            if x < HALO:
                place(right[i, :NY_LOCAL], right[12 + i, :NY_LOCAL], g, HALO + 60 + x)
    turn(x_ref, out, 80)


def halos(zb, za, left, right, roots):
    return pl.pallas_call(
        halo_kernel,
        out_shape=jax.ShapeDtypeStruct((80 * YSTEP, 128), F32),
        in_specs=[pl.BlockSpec(memory_space=VMEM)] * 4 + [pl.BlockSpec(memory_space=SMEM)],
        scratch_shapes=[VMEM((128 * YSTEP, 128), F32)],
        compiler_params=vm(16),
        cost_estimate=cost(5),
        name="halos",
    )(zb, za, left, right, roots).reshape(80, YSTEP, 128)


def split_rows(f):
    hi = f.astype(BF16).astype(F32)
    return jnp.concatenate([hi, f - hi], axis=0).astype(BF16)


def both(own, part):
    return split_rows(jnp.concatenate([own, part], axis=0))


def join_halo_kernel(full, own, part, out):
    for z in range(HALO):
        out[z] = both(own[z, :YPAD], part[z, :YPAD])
        out[HALO + 128 + z] = both(own[40 + z, :YPAD], part[40 + z, :YPAD])


def join_halo(full, own, part):
    return pl.pallas_call(
        join_halo_kernel,
        out_shape=jax.ShapeDtypeStruct(full.shape, full.dtype),
        in_specs=[
            pl.BlockSpec(memory_space=ANY),
            pl.BlockSpec(memory_space=VMEM),
            pl.BlockSpec(memory_space=VMEM),
        ],
        input_output_aliases={0: 0},
        compiler_params=vm(10),
        cost_estimate=cost(2),
        name="join_halo",
    )(full, own, part)


def placed(table_hi, table_lo, hot):
    hot = jnp.where(hot, 1.0, 0.0).astype(BF16)
    hi = jnp.dot(table_hi, hot, preferred_element_type=F32)
    lo = jnp.dot(table_lo, hot, preferred_element_type=F32)
    top = jnp.concatenate([hi, hi], axis=1)
    low = jnp.concatenate([lo, jnp.zeros_like(lo)], axis=1)
    return jnp.concatenate([top, low], axis=0).astype(BF16)


def folded(r):
    return r[:G] + r[G:]


def locate(roots, place, sizes, slot, holder):
    nx, ny, nz, bx, by, bz = sizes
    ok = jnp.int32(0)
    x0 = y0 = z0 = jnp.int32(0)
    for s in range(slot):
        def rel(dim, origin, total):
            v = roots[holder, dim, s] + HALO - origin
            return jnp.where(v < 0, v + total, jnp.where(v >= total, v - total, v))

        rx = rel(0, place[0] * bx, nx)
        mine = rx < bx
        ok = jnp.where(mine, 1, ok)
        x0 = jnp.where(mine, rx, x0)
        y0 = jnp.where(mine, rel(1, place[1] * by, ny) - HALO, y0)
        z0 = jnp.where(mine, rel(2, place[2] * bz, nz), z0)
    return ok, x0, y0, z0


def field_kernel(late, sizes, slot, n, roots, place, thi, tlo, a2_ref, full, out, t1, t2, obuf, info, sems):
    def find(j, carry):
        ok, x0, y0, z0 = locate(roots, place, sizes, slot, j)
        inside = jnp.logical_and(z0 >= HALO, z0 <= HALO + 128 - BOX)
        info[0, j] = jnp.where(inside, 0, ok) if late else jnp.where(inside, ok, 0)
        info[1, j] = x0
        info[2, j] = y0
        info[3, j] = z0
        return carry

    lax.fori_loop(0, n, find, 0)

    def out_copy(j, b):
        return pltpu.make_async_copy(obuf.at[b], out.at[j], sems.at[b])

    for b in range(G):
        t1[b * 72 + 64:b * 72 + 72, :] = jnp.zeros((8, 128), F32)

    def compute(j, b):
        x0 = info[1, j]
        y0 = info[2, j]
        z0 = info[3, j]
        k = lax.broadcasted_iota(jnp.int32, (128, 128), 0)
        col = lax.broadcasted_iota(jnp.int32, (128, 128), 1)
        half = col & 63
        near = jnp.where(col < 64, col, col - 4) - y0
        far = jnp.where(col < 64, -1, col - 124 - y0)
        hot_y = jnp.logical_and(half < NY_LOCAL, jnp.logical_or(k == near, k == far))
        a1 = placed(thi[...], tlo[...], hot_y)
        a3 = placed(thi[...], tlo[...], k == col - x0)
        a2 = a2_ref[...]
        for p in range(BOX // 2):
            rhs = jnp.concatenate([full[z0 + 2 * p], full[z0 + 2 * p + 1]], axis=1)
            t = folded(jnp.dot(a1, rhs, preferred_element_type=F32))
            t1[pl.ds(2 * p, G, stride=72), :] = t[:, :128]
            t1[pl.ds(2 * p + 1, G, stride=72), :] = t[:, 128:]
        for q in range(0, G, 2):
            f = jnp.concatenate([t1[q * 72:q * 72 + 72, :], t1[q * 72 + 72:q * 72 + 144, :]], axis=1)
            t = folded(jnp.dot(a2, split_rows(f), preferred_element_type=F32))
            t2[q * G:q * G + G, :] = t[:, :128]
            t2[q * G + G:q * G + 2 * G, :] = t[:, 128:]
        for m in range(9):
            f = t2[256 * m:256 * m + 256, :]
            hi = f.astype(BF16)
            lo = (f - hi.astype(F32)).astype(BF16)
            rhs = jnp.concatenate([hi, lo], axis=1)
            r = lax.dot_general(a3, rhs, (((1,), (1,)), ((), ())), preferred_element_type=F32)
            t = folded(r)
            obuf[b, pl.ds(2 * m, G, stride=18), :] = t[:, :128]
            obuf[b, pl.ds(2 * m + 1, G, stride=18), :] = t[:, 128:]

    def drain(j, b):
        @pl.when(info[0, j] == 1)
        def _():
            out_copy(0, b).wait()

    def step(j, carry):
        b = lax.rem(j, 2)

        @pl.when(j >= 2)
        def _():
            drain(j - 2, b)

        @pl.when(info[0, j] == 1)
        def _():
            compute(j, b)
            out_copy(j, b).start()

        return carry

    lax.fori_loop(0, n, step, 0)
    drain(n - 2, (n - 2) % 2)
    drain(n - 1, (n - 1) % 2)


def fields(sizes, slot, n, roots, place, thi, tlo, a2, full, done=None):
    smem = pl.BlockSpec(memory_space=SMEM)
    vmem = pl.BlockSpec(memory_space=VMEM)
    hbm = pl.BlockSpec(memory_space=ANY)
    late = done is not None
    out = jax.ShapeDtypeStruct((n, ROWS, 128), F32)

    def kernel(*refs):
        if late:
            field_kernel(True, sizes, slot, n, *refs[:6], *refs[7:])
        else:
            field_kernel(False, sizes, slot, n, *refs[:7], *refs[8:])

    args = (roots, place, thi, tlo, a2, full) + ((done,) if late else ())
    return pl.pallas_call(
        kernel,
        out_shape=(out,) if late else (out, jax.ShapeDtypeStruct(full.shape, full.dtype)),
        in_specs=[smem, smem, vmem, vmem, vmem, vmem] + [hbm] * late,
        out_specs=(hbm,) if late else (hbm, hbm),
        scratch_shapes=[
            VMEM((G * 72, 128), F32),
            VMEM((G * G, 128), F32),
            VMEM((2, ROWS, 128), F32),
            SMEM((4, n), jnp.int32),
            pltpu.SemaphoreType.DMA((2,)),
        ],
        input_output_aliases={6: 0} if late else {5: 1},
        compiler_params=vm(8),
        cost_estimate=cost(FIELD_COST * n),
        name="fields",
    )(*args)


def pick_kernel(sizes, slot, n, own_root, parts, out, buf, sems):
    nx, bx = sizes[0], sizes[3]
    for s in range(slot):
        r = own_root[0, s] + HALO
        r = jnp.where(r >= nx, r - nx, r)

        def scan(j, anchor):
            return jnp.where(r >= j * bx, j, anchor)

        anchor = lax.fori_loop(0, n, scan, jnp.int32(0), unroll=True)
        pltpu.make_async_copy(parts.at[anchor], buf.at[s], sems.at[s]).start()
    for s in range(slot):
        pltpu.make_async_copy(parts.at[0], buf.at[s], sems.at[s]).wait()
        out[pl.ds(s, ROWS, stride=slot), :] = buf[s]


def pick(sizes, slot, n, own_root, parts):
    def kernel(*refs):
        pick_kernel(sizes, slot, n, *refs)

    return pl.pallas_call(
        kernel,
        out_shape=jax.ShapeDtypeStruct((ROWS * slot, 128), F32),
        in_specs=[pl.BlockSpec(memory_space=SMEM), pl.BlockSpec(memory_space=ANY)],
        scratch_shapes=[VMEM((slot, ROWS, 128), F32), pltpu.SemaphoreType.DMA((slot,))],
        compiler_params=vm(8),
        name="pick",
    )(own_root, parts)


def program(potential, frag_root):
    bx, by, bz = potential.shape
    groups = lax.axis_size("gx")
    zs = lax.axis_size("gz")
    sizes = (bx * groups, by * lax.axis_size("gy"), bz * zs, bx, by, bz)
    slot = frag_root.shape[1]
    place = jnp.stack([lax.axis_index("gx"), lax.axis_index("gy"), lax.axis_index("gz")]).astype(jnp.int32)

    def move(v, sx, sz):
        axis, count, by = ("gx", groups, sx) if sx else ("gz", zs, sz)
        return lax.ppermute(v, axis, [(i, (i + by) % count) for i in range(count)])

    before = move(potential[bx - HALO:], 1, 0)
    after = move(potential[:HALO], -1, 0)
    za, zb = pack(potential)
    got_zb = move(zb, 0, 1)
    got_za = move(za, 0, -1)
    left = move(jnp.concatenate([got_zb[8:], got_za[8:]], axis=0), 1, 0)
    right = move(jnp.concatenate([got_zb[:12], got_za[:12]], axis=0), -1, 0)
    roots = lax.all_to_all(
        jnp.broadcast_to(frag_root[None], (groups, 3, slot)), "gx", 0, 0, tiled=True
    )

    swap = [(0, 1), (1, 0)]
    part_own = lax.ppermute(potential, "gy", swap)
    part_after = lax.ppermute(after, "gy", swap)
    part_before = lax.ppermute(before, "gy", swap)
    full = middle(before, potential, after, part_before, part_own, part_after, zb)
    own_h = halos(got_zb, got_za, left, right, roots)
    part_h = lax.ppermute(own_h, "gy", swap)

    table = interp_matrix()
    hi = np.asarray(table.astype(BF16))
    lo = (table - hi.astype(np.float32)).astype(BF16)
    thi = np.zeros((G, 128), BF16)
    tlo = np.zeros((G, 128), BF16)
    thi[:, :BOX] = hi
    tlo[:, :BOX] = lo
    a2 = np.zeros((2 * G, 144), BF16)
    a2[:G, :BOX] = hi
    a2[:G, 72:72 + BOX] = hi
    a2[G:, :BOX] = lo

    done, full = fields(sizes, slot, groups, roots, place, thi, tlo, a2, full)
    full = join_halo(full, own_h, part_h)
    (done,) = fields(sizes, slot, groups, roots, place, thi, tlo, a2, full, done)
    parts = lax.all_to_all(done, "gx", 0, 0, tiled=True)
    out = pick(sizes, slot, groups, frag_root, parts)
    return jnp.transpose(out.reshape(ROWS, slot, 128), (1, 0, 2)).reshape(slot, ROWS * 128)


def solution(mesh):
    return jax.shard_map(
        program,
        mesh=mesh,
        in_specs=(P("gx", "gy", "gz"), P(None, ("gx", "gy", "gz"))),
        out_specs=P(("gx", "gy", "gz"), None),
        check_vma=False,
    )
```

```python
import math

import jax
import jax.numpy as jnp
import numpy as np
from jax import lax
from jax.experimental import pallas as pl
from jax.experimental.pallas import tpu as pltpu
from jax.sharding import PartitionSpec as P


G = 48
BOX = 68
HALO = 34
NY_LOCAL = 60
YPAD = 64
YSTEP = 72
T1STEP = 76
ROWS = G * G * G // 128
PLANE = G * G // 128
KEPT = (G - 1) * PLANE
SENT = KEPT + 2
F32 = jnp.float32
BF16 = jnp.bfloat16
MID_COST = 10
FIELD_COST = 3
ANY = pl.ANY
VMEM = pltpu.VMEM
SMEM = pltpu.SMEM


def interp_matrix():
    a = np.arange(G, dtype=np.float64)[:, None]
    x = np.arange(BOX, dtype=np.float64)[None, :]
    total = np.ones((G, BOX))
    for k in range(1, G // 2):
        total = total + 2.0 * np.cos(2.0 * math.pi * k * (a / G - x / BOX))
    return (total / BOX).astype(np.float32)


def cost(us):
    return pl.CostEstimate(flops=int(us * 1e9), bytes_accessed=0, transcendentals=0)


def vm(limit=48):
    return pltpu.CompilerParams(vmem_limit_bytes=limit << 20)


def pack_rows(p_ref, side, i, lane):
    base, first = (0, 40) if side == 0 else (128 - HALO, 0)
    rows = []
    for g in range(3):
        v = p_ref[3 * i + g]
        shift = (first + HALO * g - base) % 128
        rows.append(pltpu.roll(v, shift, 1) if shift else v)
    at = jnp.where(lane < first, lane + 128 - first, lane - first)
    return jnp.where(at < HALO, rows[0], jnp.where(at < 2 * HALO, rows[1], rows[2]))


def pack_kernel(p_ref, za, zb):
    lane = lax.broadcasted_iota(jnp.int32, (NY_LOCAL, 128), 1)
    for i in range(20):
        za[i, :NY_LOCAL] = pack_rows(p_ref, 0, i, lane)
        zb[i, :NY_LOCAL] = pack_rows(p_ref, 1, i, lane)


def pack(p):
    big = jax.ShapeDtypeStruct((20, YPAD, 128), F32)
    return pl.pallas_call(
        pack_kernel,
        out_shape=(big, big),
        compiler_params=vm(10),
        name="pack",
    )(p)


def turn(src, out, count):
    r = lax.broadcasted_iota(jnp.int32, (count, 256), 0)
    c = lax.broadcasted_iota(jnp.int32, (count, 256), 1) & 127
    pick_z = jnp.where(r == c, 1.0, 0.0).astype(BF16)
    for y in range(0, NY_LOCAL, 2):
        m = jnp.concatenate([src[pl.ds(y + k, 128, stride=YSTEP), :] for k in range(2)], axis=0)
        hi = m.astype(BF16)
        lo = (m - hi.astype(F32)).astype(BF16)
        pair = jnp.concatenate([hi, lo], axis=1)
        t = lax.dot_general(pick_z, pair, (((1,), (1,)), ((), ())), preferred_element_type=F32)
        out[pl.ds(y, count, stride=YSTEP), :] = t[:, :128]
        out[pl.ds(y + 1, count, stride=YSTEP), :] = t[:, 128:]
    for y in range(NY_LOCAL, YPAD):
        out[pl.ds(y, count, stride=YSTEP), :] = jnp.zeros((count, 128), F32)


def mid_kernel(before, own, after, part_before, part_own, part_after, packed, out, x_ref, t_own, t_part):
    for refs, turned in (((before, own, after), t_own), ((part_before, part_own, part_after), t_part)):
        for ref, first, n in zip(refs, (0, HALO, HALO + 60), (HALO, 60, HALO)):
            for i in range(n):
                x_ref[pl.ds(YSTEP * (first + i), NY_LOCAL), :] = ref[i]
        turn(x_ref, turned, 128)

    def step(z, carry):
        rows = pl.ds(pl.multiple_of(z * YSTEP, 8), YPAD)
        out[HALO + z] = both(t_own[rows, :], t_part[rows, :])
        return carry

    lax.fori_loop(0, 128, step, 0, unroll=4)


def middle(before, own, after, part_before, part_own, part_after, packed):
    return pl.pallas_call(
        mid_kernel,
        out_shape=jax.ShapeDtypeStruct((128 + 2 * HALO, 4 * YPAD, 128), BF16),
        in_specs=[pl.BlockSpec(memory_space=VMEM)] * 6 + [pl.BlockSpec(memory_space=ANY)],
        scratch_shapes=[VMEM((128 * YSTEP, 128), F32)] * 3,
        compiler_params=vm(40),
        cost_estimate=cost(MID_COST),
        name="middle",
    )(before, own, after, part_before, part_own, part_after, packed)


def halo_kernel(zb, za, left, right, roots, out, x_ref):
    lane = lax.broadcasted_iota(jnp.int32, (NY_LOCAL, 128), 1)

    def place(b, a, g, row):
        mine = jnp.logical_and(lane >= HALO * g, lane < HALO * g + HALO)
        v = jnp.where(mine, b, a)
        x_ref[pl.ds(YSTEP * row, NY_LOCAL), :] = pltpu.roll(v, 128 - HALO * g, 1) if g else v

    for g in range(3):
        for i in range(20):
            place(zb[i, :NY_LOCAL], za[i, :NY_LOCAL], g, HALO + 3 * i + g)
        for i in range(12):
            x = 3 * i + g - 2
            if x >= 0:
                place(left[i, :NY_LOCAL], left[12 + i, :NY_LOCAL], g, x)
            x = 3 * i + g
            if x < HALO:
                place(right[i, :NY_LOCAL], right[12 + i, :NY_LOCAL], g, HALO + 60 + x)
    turn(x_ref, out, 80)


def halos(zb, za, left, right, roots):
    return pl.pallas_call(
        halo_kernel,
        out_shape=jax.ShapeDtypeStruct((80 * YSTEP, 128), F32),
        in_specs=[pl.BlockSpec(memory_space=VMEM)] * 4 + [pl.BlockSpec(memory_space=SMEM)],
        scratch_shapes=[VMEM((128 * YSTEP, 128), F32)],
        compiler_params=vm(16),
        cost_estimate=cost(5),
        name="halos",
    )(zb, za, left, right, roots).reshape(80, YSTEP, 128)


def split_rows(f):
    hi = f.astype(BF16).astype(F32)
    return jnp.concatenate([hi, f - hi], axis=0).astype(BF16)


def both(own, part):
    return split_rows(jnp.concatenate([own, part], axis=0))


def join_halo_kernel(full, own, part, out):
    for z in range(HALO):
        out[z] = both(own[z, :YPAD], part[z, :YPAD])
        out[HALO + 128 + z] = both(own[40 + z, :YPAD], part[40 + z, :YPAD])


def join_halo(full, own, part):
    return pl.pallas_call(
        join_halo_kernel,
        out_shape=jax.ShapeDtypeStruct(full.shape, full.dtype),
        in_specs=[
            pl.BlockSpec(memory_space=ANY),
            pl.BlockSpec(memory_space=VMEM),
            pl.BlockSpec(memory_space=VMEM),
        ],
        input_output_aliases={0: 0},
        compiler_params=vm(10),
        cost_estimate=cost(2),
        name="join_halo",
    )(full, own, part)


def placed(table_hi, table_lo, hot):
    hot = jnp.where(hot, 1.0, 0.0).astype(BF16)
    hi = jnp.dot(table_hi, hot, preferred_element_type=F32)
    lo = jnp.dot(table_lo, hot, preferred_element_type=F32)
    top = jnp.concatenate([hi, hi], axis=1)
    low = jnp.concatenate([lo, jnp.zeros_like(lo)], axis=1)
    return jnp.concatenate([top, low], axis=0).astype(BF16)


def folded(r):
    return r[:G] + r[G:]


def locate(roots, place, sizes, slot, holder):
    nx, ny, nz, bx, by, bz = sizes
    ok = jnp.int32(0)
    x0 = y0 = z0 = jnp.int32(0)
    for s in range(slot):
        def rel(dim, origin, total):
            v = roots[holder, dim, s] + HALO - origin
            return jnp.where(v < 0, v + total, jnp.where(v >= total, v - total, v))

        rx = rel(0, place[0] * bx, nx)
        mine = rx < bx
        ok = jnp.where(mine, 1, ok)
        x0 = jnp.where(mine, rx, x0)
        y0 = jnp.where(mine, rel(1, place[1] * by, ny) - HALO, y0)
        z0 = jnp.where(mine, rel(2, place[2] * bz, nz), z0)
    return ok, x0, y0, z0


def field_kernel(late, sizes, slot, n, roots, place, thi, tlo, a2_ref, full, out, t1, t2, obuf, info, sems):
    def find(j, carry):
        ok, x0, y0, z0 = locate(roots, place, sizes, slot, j)
        inside = jnp.logical_and(z0 >= HALO, z0 <= HALO + 128 - BOX)
        info[0, j] = jnp.where(inside, 0, ok) if late else jnp.where(inside, ok, 0)
        info[1, j] = x0
        info[2, j] = y0
        info[3, j] = z0
        return carry

    lax.fori_loop(0, n, find, 0)

    def out_copy(j, b):
        return pltpu.make_async_copy(obuf.at[b], out.at[j], sems.at[b])

    for b in range(G):
        t1[b * T1STEP + 64:b * T1STEP + 72, :] = jnp.zeros((8, 128), F32)

    def compute(j, b):
        x0 = info[1, j]
        y0 = info[2, j]
        z0 = info[3, j]
        k = lax.broadcasted_iota(jnp.int32, (128, 128), 0)
        col = lax.broadcasted_iota(jnp.int32, (128, 128), 1)
        half = col & 63
        near = jnp.where(col < 64, col, col - 4) - y0
        far = jnp.where(col < 64, -1, col - 124 - y0)
        hot_y = jnp.logical_and(half < NY_LOCAL, jnp.logical_or(k == near, k == far))
        a1 = placed(thi[...], tlo[...], hot_y)
        a3 = placed(thi[...], tlo[...], k == col - x0)
        a2 = a2_ref[...]
        for p in range(BOX // 2):
            rhs = jnp.concatenate([full[z0 + 2 * p], full[z0 + 2 * p + 1]], axis=1)
            t = folded(jnp.dot(a1, rhs, preferred_element_type=F32))
            t1[pl.ds(2 * p, G, stride=T1STEP), :] = t[:, :128]
            t1[pl.ds(2 * p + 1, G, stride=T1STEP), :] = t[:, 128:]
        for q in range(0, G, 2):
            f = jnp.concatenate([t1[q * T1STEP:q * T1STEP + 72, :], t1[q * T1STEP + T1STEP:q * T1STEP + T1STEP + 72, :]], axis=1)
            t = folded(jnp.dot(a2, split_rows(f), preferred_element_type=F32))
            t2[q * G:q * G + G, :] = t[:, :128]
            t2[q * G + G:q * G + 2 * G, :] = t[:, 128:]
        for m in range(9):
            f = t2[256 * m:256 * m + 256, :]
            hi = f.astype(BF16)
            lo = (f - hi.astype(F32)).astype(BF16)
            rhs = jnp.concatenate([hi, lo], axis=1)
            r = lax.dot_general(a3, rhs, (((1,), (1,)), ((), ())), preferred_element_type=F32)
            t = folded(r)
            obuf[b, pl.ds(2 * m, G - 1, stride=PLANE), :] = t[:G - 1, :128]
            obuf[b, pl.ds(2 * m + 1, G - 1, stride=PLANE), :] = t[:G - 1, 128:]

    def drain(j, b):
        @pl.when(info[0, j] == 1)
        def _():
            out_copy(0, b).wait()

    def step(j, carry):
        b = lax.rem(j, 2)

        @pl.when(j >= 2)
        def _():
            drain(j - 2, b)

        @pl.when(info[0, j] == 1)
        def _():
            compute(j, b)
            out_copy(j, b).start()

        return carry

    lax.fori_loop(0, n, step, 0)
    drain(n - 2, (n - 2) % 2)
    drain(n - 1, (n - 1) % 2)


def fields(sizes, slot, n, roots, place, thi, tlo, a2, full, done=None):
    smem = pl.BlockSpec(memory_space=SMEM)
    vmem = pl.BlockSpec(memory_space=VMEM)
    hbm = pl.BlockSpec(memory_space=ANY)
    late = done is not None
    out = jax.ShapeDtypeStruct((n, SENT, 128), F32)

    def kernel(*refs):
        if late:
            field_kernel(True, sizes, slot, n, *refs[:6], *refs[7:])
        else:
            field_kernel(False, sizes, slot, n, *refs[:7], *refs[8:])

    args = (roots, place, thi, tlo, a2, full) + ((done,) if late else ())
    return pl.pallas_call(
        kernel,
        out_shape=(out,) if late else (out, jax.ShapeDtypeStruct(full.shape, full.dtype)),
        in_specs=[smem, smem, vmem, vmem, vmem, vmem] + [hbm] * late,
        out_specs=(hbm,) if late else (hbm, hbm),
        scratch_shapes=[
            VMEM((G * T1STEP, 128), F32),
            VMEM((G * G, 128), F32),
            VMEM((2, SENT, 128), F32),
            SMEM((4, n), jnp.int32),
            pltpu.SemaphoreType.DMA((2,)),
        ],
        input_output_aliases={6: 0} if late else {5: 1},
        compiler_params=vm(8),
        cost_estimate=cost(FIELD_COST * n),
        name="fields",
    )(*args)


def pick_kernel(sizes, slot, n, own_root, parts, out, buf, sems):
    nx, bx = sizes[0], sizes[3]
    for s in range(slot):
        r = own_root[0, s] + HALO
        r = jnp.where(r >= nx, r - nx, r)

        def scan(j, anchor):
            return jnp.where(r >= j * bx, j, anchor)

        anchor = lax.fori_loop(0, n, scan, jnp.int32(0), unroll=True)
        pltpu.make_async_copy(parts.at[anchor], buf.at[s], sems.at[s]).start()
    for s in range(slot):
        pltpu.make_async_copy(parts.at[0], buf.at[s], sems.at[s]).wait()
        out[pl.ds(s, KEPT, stride=slot), :] = buf[s, :KEPT]
        last = buf[s, :PLANE]
        for a in range(1, G - 1):
            plane = buf[s, a * PLANE:(a + 1) * PLANE]
            last = last - plane if a % 2 else last + plane
        out[pl.ds(KEPT * slot + s, PLANE, stride=slot), :] = last


def pick(sizes, slot, n, own_root, parts):
    def kernel(*refs):
        pick_kernel(sizes, slot, n, *refs)

    return pl.pallas_call(
        kernel,
        out_shape=jax.ShapeDtypeStruct((ROWS * slot, 128), F32),
        in_specs=[pl.BlockSpec(memory_space=SMEM), pl.BlockSpec(memory_space=ANY)],
        scratch_shapes=[VMEM((slot, SENT, 128), F32), pltpu.SemaphoreType.DMA((slot,))],
        compiler_params=vm(8),
        name="pick",
    )(own_root, parts)


def program(potential, frag_root):
    bx, by, bz = potential.shape
    groups = lax.axis_size("gx")
    zs = lax.axis_size("gz")
    sizes = (bx * groups, by * lax.axis_size("gy"), bz * zs, bx, by, bz)
    slot = frag_root.shape[1]
    place = jnp.stack([lax.axis_index("gx"), lax.axis_index("gy"), lax.axis_index("gz")]).astype(jnp.int32)

    def move(v, sx, sz):
        axis, count, by = ("gx", groups, sx) if sx else ("gz", zs, sz)
        return lax.ppermute(v, axis, [(i, (i + by) % count) for i in range(count)])

    before = move(potential[bx - HALO:], 1, 0)
    after = move(potential[:HALO], -1, 0)
    za, zb = pack(potential)
    got_zb = move(zb, 0, 1)
    got_za = move(za, 0, -1)
    left = move(jnp.concatenate([got_zb[8:], got_za[8:]], axis=0), 1, 0)
    right = move(jnp.concatenate([got_zb[:12], got_za[:12]], axis=0), -1, 0)
    roots = lax.all_to_all(
        jnp.broadcast_to(frag_root[None], (groups, 3, slot)), "gx", 0, 0, tiled=True
    )

    swap = [(0, 1), (1, 0)]
    part_own = lax.ppermute(potential, "gy", swap)
    part_after = lax.ppermute(after, "gy", swap)
    part_before = lax.ppermute(before, "gy", swap)
    full = middle(before, potential, after, part_before, part_own, part_after, zb)
    own_h = halos(got_zb, got_za, left, right, roots)
    part_h = lax.ppermute(own_h, "gy", swap)

    table = interp_matrix()
    hi = np.asarray(table.astype(BF16))
    lo = (table - hi.astype(np.float32)).astype(BF16)
    thi = np.zeros((G, 128), BF16)
    tlo = np.zeros((G, 128), BF16)
    thi[:, :BOX] = hi
    tlo[:, :BOX] = lo
    a2 = np.zeros((2 * G, 144), BF16)
    a2[:G, :BOX] = hi
    a2[:G, 72:72 + BOX] = hi
    a2[G:, :BOX] = lo

    done, full = fields(sizes, slot, groups, roots, place, thi, tlo, a2, full)
    full = join_halo(full, own_h, part_h)
    (done,) = fields(sizes, slot, groups, roots, place, thi, tlo, a2, full, done)
    parts = lax.all_to_all(done, "gx", 0, 0, tiled=True)
    out = pick(sizes, slot, groups, frag_root, parts)
    return jnp.transpose(out.reshape(ROWS, slot, 128), (1, 0, 2)).reshape(slot, ROWS * 128)


def solution(mesh):
    return jax.shard_map(
        program,
        mesh=mesh,
        in_specs=(P("gx", "gy", "gz"), P(None, ("gx", "gy", "gz"))),
        out_specs=P(("gx", "gy", "gz"), None),
        check_vma=False,
    )
```

```python
import math

import jax
import jax.numpy as jnp
import numpy as np
from jax import lax
from jax.experimental import pallas as pl
from jax.experimental.pallas import tpu as pltpu
from jax.sharding import PartitionSpec as P


G = 48
BOX = 68
HALO = 34
NY_LOCAL = 60
YPAD = 64
YSTEP = 72
T1STEP = 76
ROWS = G * G * G // 128
PLANE = G * G // 128
KEPT = (G - 1) * PLANE
SENT = KEPT + 2
F32 = jnp.float32
BF16 = jnp.bfloat16
MID_COST = 10
FIELD_COST = 3
ANY = pl.ANY
VMEM = pltpu.VMEM
SMEM = pltpu.SMEM


def interp_matrix():
    a = np.arange(G, dtype=np.float64)[:, None]
    x = np.arange(BOX, dtype=np.float64)[None, :]
    total = np.ones((G, BOX))
    for k in range(1, G // 2):
        total = total + 2.0 * np.cos(2.0 * math.pi * k * (a / G - x / BOX))
    return (total / BOX).astype(np.float32)


def cost(us):
    return pl.CostEstimate(flops=int(us * 1e9), bytes_accessed=0, transcendentals=0)


def vm(limit=48):
    return pltpu.CompilerParams(vmem_limit_bytes=limit << 20)


def pack_rows(p_ref, side, i, lane):
    base, first = (0, 40) if side == 0 else (128 - HALO, 0)
    rows = []
    for g in range(3):
        v = p_ref[3 * i + g]
        shift = (first + HALO * g - base) % 128
        rows.append(pltpu.roll(v, shift, 1) if shift else v)
    at = jnp.where(lane < first, lane + 128 - first, lane - first)
    return jnp.where(at < HALO, rows[0], jnp.where(at < 2 * HALO, rows[1], rows[2]))


def pack_kernel(p_ref, za, zb):
    lane = lax.broadcasted_iota(jnp.int32, (NY_LOCAL, 128), 1)
    for i in range(20):
        za[i, :NY_LOCAL] = pack_rows(p_ref, 0, i, lane)
        zb[i, :NY_LOCAL] = pack_rows(p_ref, 1, i, lane)


def pack(p):
    big = jax.ShapeDtypeStruct((20, YPAD, 128), F32)
    return pl.pallas_call(
        pack_kernel,
        out_shape=(big, big),
        compiler_params=vm(10),
        name="pack",
    )(p)


def turn(src, out, count):
    r = lax.broadcasted_iota(jnp.int32, (count, 256), 0)
    c = lax.broadcasted_iota(jnp.int32, (count, 256), 1) & 127
    pick_z = jnp.where(r == c, 1.0, 0.0).astype(BF16)
    for y in range(0, NY_LOCAL, 2):
        m = jnp.concatenate([src[pl.ds(y + k, 128, stride=YSTEP), :] for k in range(2)], axis=0)
        hi = m.astype(BF16)
        lo = (m - hi.astype(F32)).astype(BF16)
        pair = jnp.concatenate([hi, lo], axis=1)
        t = lax.dot_general(pick_z, pair, (((1,), (1,)), ((), ())), preferred_element_type=F32)
        out[pl.ds(y, count, stride=YSTEP), :] = t[:, :128]
        out[pl.ds(y + 1, count, stride=YSTEP), :] = t[:, 128:]
    for y in range(NY_LOCAL, YPAD):
        out[pl.ds(y, count, stride=YSTEP), :] = jnp.zeros((count, 128), F32)


def mid_kernel(before, own, after, part_before, part_own, part_after, packed, out, x_ref, t_own, t_part):
    for refs, turned in (((before, own, after), t_own), ((part_before, part_own, part_after), t_part)):
        for ref, first, n in zip(refs, (0, HALO, HALO + 60), (HALO, 60, HALO)):
            for i in range(n):
                x_ref[pl.ds(YSTEP * (first + i), NY_LOCAL), :] = ref[i]
        turn(x_ref, turned, 128)

    def step(z, carry):
        rows = pl.ds(pl.multiple_of(z * YSTEP, 8), YPAD)
        out[HALO + z] = both(t_own[rows, :], t_part[rows, :])
        return carry

    lax.fori_loop(0, 128, step, 0, unroll=4)


def middle(before, own, after, part_before, part_own, part_after, packed):
    return pl.pallas_call(
        mid_kernel,
        out_shape=jax.ShapeDtypeStruct((128 + 2 * HALO, 4 * YPAD, 128), BF16),
        in_specs=[pl.BlockSpec(memory_space=VMEM)] * 6 + [pl.BlockSpec(memory_space=ANY)],
        scratch_shapes=[VMEM((128 * YSTEP, 128), F32)] * 3,
        compiler_params=vm(40),
        cost_estimate=cost(MID_COST),
        name="middle",
    )(before, own, after, part_before, part_own, part_after, packed)


def halo_kernel(zb, za, left, right, roots, out, x_ref):
    lane = lax.broadcasted_iota(jnp.int32, (NY_LOCAL, 128), 1)

    def place(b, a, g, row):
        mine = jnp.logical_and(lane >= HALO * g, lane < HALO * g + HALO)
        v = jnp.where(mine, b, a)
        x_ref[pl.ds(YSTEP * row, NY_LOCAL), :] = pltpu.roll(v, 128 - HALO * g, 1) if g else v

    for g in range(3):
        for i in range(20):
            place(zb[i, :NY_LOCAL], za[i, :NY_LOCAL], g, HALO + 3 * i + g)
        for i in range(12):
            x = 3 * i + g - 2
            if x >= 0:
                place(left[i, :NY_LOCAL], left[12 + i, :NY_LOCAL], g, x)
            x = 3 * i + g
            if x < HALO:
                place(right[i, :NY_LOCAL], right[12 + i, :NY_LOCAL], g, HALO + 60 + x)
    turn(x_ref, out, 80)


def halos(zb, za, left, right, roots):
    return pl.pallas_call(
        halo_kernel,
        out_shape=jax.ShapeDtypeStruct((80 * YSTEP, 128), F32),
        in_specs=[pl.BlockSpec(memory_space=VMEM)] * 4 + [pl.BlockSpec(memory_space=SMEM)],
        scratch_shapes=[VMEM((128 * YSTEP, 128), F32)],
        compiler_params=vm(16),
        cost_estimate=cost(5),
        name="halos",
    )(zb, za, left, right, roots).reshape(80, YSTEP, 128)


def split_rows(f):
    hi = f.astype(BF16).astype(F32)
    return jnp.concatenate([hi, f - hi], axis=0).astype(BF16)


def both(own, part):
    return split_rows(jnp.concatenate([own, part], axis=0))


def join_halo_kernel(full, own, part, out):
    for z in range(HALO):
        out[z] = both(own[z, :YPAD], part[z, :YPAD])
        out[HALO + 128 + z] = both(own[40 + z, :YPAD], part[40 + z, :YPAD])


def join_halo(full, own, part):
    return pl.pallas_call(
        join_halo_kernel,
        out_shape=jax.ShapeDtypeStruct(full.shape, full.dtype),
        in_specs=[
            pl.BlockSpec(memory_space=ANY),
            pl.BlockSpec(memory_space=VMEM),
            pl.BlockSpec(memory_space=VMEM),
        ],
        input_output_aliases={0: 0},
        compiler_params=vm(10),
        cost_estimate=cost(2),
        name="join_halo",
    )(full, own, part)


def placed(table_hi, table_lo, hot):
    hot = jnp.where(hot, 1.0, 0.0).astype(BF16)
    hi = jnp.dot(table_hi, hot, preferred_element_type=F32)
    lo = jnp.dot(table_lo, hot, preferred_element_type=F32)
    top = jnp.concatenate([hi, hi], axis=1)
    low = jnp.concatenate([lo, jnp.zeros_like(lo)], axis=1)
    return jnp.concatenate([top, low], axis=0).astype(BF16)


def folded(r):
    return r[:G] + r[G:]


def locate(roots, place, sizes, slot, holder):
    nx, ny, nz, bx, by, bz = sizes
    ok = jnp.int32(0)
    x0 = y0 = z0 = jnp.int32(0)
    for s in range(slot):
        def rel(dim, origin, total):
            v = roots[holder, dim, s] + HALO - origin
            return jnp.where(v < 0, v + total, jnp.where(v >= total, v - total, v))

        rx = rel(0, place[0] * bx, nx)
        mine = rx < bx
        ok = jnp.where(mine, 1, ok)
        x0 = jnp.where(mine, rx, x0)
        y0 = jnp.where(mine, rel(1, place[1] * by, ny) - HALO, y0)
        z0 = jnp.where(mine, rel(2, place[2] * bz, nz), z0)
    return ok, x0, y0, z0


def field_kernel(late, sizes, slot, n, roots, place, thi, tlo, a2_ref, full, out, t1, t2, obuf, info, sems):
    def find(j, carry):
        ok, x0, y0, z0 = locate(roots, place, sizes, slot, j)
        inside = jnp.logical_and(z0 >= HALO, z0 <= HALO + 128 - BOX)
        info[0, j] = jnp.where(inside, 0, ok) if late else jnp.where(inside, ok, 0)
        info[1, j] = x0
        info[2, j] = y0
        info[3, j] = z0
        return carry

    lax.fori_loop(0, n, find, 0)

    def out_copy(j, b):
        return pltpu.make_async_copy(obuf.at[b, pl.ds(0, SENT)], out.at[j], sems.at[b])

    for b in range(G):
        t1[b * T1STEP + 64:b * T1STEP + 72, :] = jnp.zeros((8, 128), F32)

    def compute(j, b):
        x0 = info[1, j]
        y0 = info[2, j]
        z0 = info[3, j]
        k = lax.broadcasted_iota(jnp.int32, (128, 128), 0)
        col = lax.broadcasted_iota(jnp.int32, (128, 128), 1)
        half = col & 63
        near = jnp.where(col < 64, col, col - 4) - y0
        far = jnp.where(col < 64, -1, col - 124 - y0)
        hot_y = jnp.logical_and(half < NY_LOCAL, jnp.logical_or(k == near, k == far))
        a1 = placed(thi[...], tlo[...], hot_y)
        a3 = placed(thi[...], tlo[...], k == col - x0)
        a2 = a2_ref[...]
        for p in range(BOX // 2):
            rhs = jnp.concatenate([full[z0 + 2 * p], full[z0 + 2 * p + 1]], axis=1)
            t = folded(jnp.dot(a1, rhs, preferred_element_type=F32))
            t1[pl.ds(2 * p, G, stride=T1STEP), :] = t[:, :128]
            t1[pl.ds(2 * p + 1, G, stride=T1STEP), :] = t[:, 128:]
        for q in range(0, G, 2):
            f = jnp.concatenate([t1[q * T1STEP:q * T1STEP + 72, :], t1[q * T1STEP + T1STEP:q * T1STEP + T1STEP + 72, :]], axis=1)
            t = folded(jnp.dot(a2, split_rows(f), preferred_element_type=F32))
            t2[q * G:q * G + G, :] = t[:, :128]
            t2[q * G + G:q * G + 2 * G, :] = t[:, 128:]
        for m in range(9):
            f = t2[256 * m:256 * m + 256, :]
            hi = f.astype(BF16)
            lo = (f - hi.astype(F32)).astype(BF16)
            rhs = jnp.concatenate([hi, lo], axis=1)
            r = lax.dot_general(a3, rhs, (((1,), (1,)), ((), ())), preferred_element_type=F32)
            t = folded(r)
            obuf[b, pl.ds(2 * m, G - 1, stride=PLANE), :] = t[:G - 1, :128]
            obuf[b, pl.ds(2 * m + 1, G - 1, stride=PLANE), :] = t[:G - 1, 128:]

    def drain(j, b):
        @pl.when(info[0, j] == 1)
        def _():
            out_copy(0, b).wait()

    def step(j, carry):
        b = lax.rem(j, 2)

        @pl.when(j >= 2)
        def _():
            drain(j - 2, b)

        @pl.when(info[0, j] == 1)
        def _():
            compute(j, b)
            out_copy(j, b).start()

        return carry

    lax.fori_loop(0, n, step, 0)
    drain(n - 2, (n - 2) % 2)
    drain(n - 1, (n - 1) % 2)


def fields(sizes, slot, n, roots, place, thi, tlo, a2, full, done=None):
    smem = pl.BlockSpec(memory_space=SMEM)
    vmem = pl.BlockSpec(memory_space=VMEM)
    hbm = pl.BlockSpec(memory_space=ANY)
    late = done is not None
    out = jax.ShapeDtypeStruct((n, SENT, 128), F32)

    def kernel(*refs):
        if late:
            field_kernel(True, sizes, slot, n, *refs[:6], *refs[7:])
        else:
            field_kernel(False, sizes, slot, n, *refs[:7], *refs[8:])

    args = (roots, place, thi, tlo, a2, full) + ((done,) if late else ())
    return pl.pallas_call(
        kernel,
        out_shape=(out,) if late else (out, jax.ShapeDtypeStruct(full.shape, full.dtype)),
        in_specs=[smem, smem, vmem, vmem, vmem, vmem] + [hbm] * late,
        out_specs=(hbm,) if late else (hbm, hbm),
        scratch_shapes=[
            VMEM((G * T1STEP, 128), F32),
            VMEM((G * G, 128), F32),
            VMEM((2, ROWS, 128), F32),
            SMEM((4, n), jnp.int32),
            pltpu.SemaphoreType.DMA((2,)),
        ],
        input_output_aliases={6: 0} if late else {5: 1},
        compiler_params=vm(8),
        cost_estimate=cost(FIELD_COST * n),
        name="fields",
    )(*args)


def pick_kernel(sizes, slot, n, own_root, parts, out, buf, sems):
    nx, bx = sizes[0], sizes[3]
    for s in range(slot):
        r = own_root[0, s] + HALO
        r = jnp.where(r >= nx, r - nx, r)

        def scan(j, anchor):
            return jnp.where(r >= j * bx, j, anchor)

        anchor = lax.fori_loop(0, n, scan, jnp.int32(0), unroll=True)
        pltpu.make_async_copy(parts.at[anchor], buf.at[s, pl.ds(0, SENT)], sems.at[s]).start()
    for s in range(slot):
        pltpu.make_async_copy(parts.at[0], buf.at[s, pl.ds(0, SENT)], sems.at[s]).wait()
        last = buf[s, :PLANE]
        for a in range(1, G - 1):
            plane = buf[s, a * PLANE:(a + 1) * PLANE]
            last = last - plane if a % 2 else last + plane
        buf[s, KEPT:ROWS] = last
        out[pl.ds(s, ROWS, stride=slot), :] = buf[s, :ROWS]


def pick(sizes, slot, n, own_root, parts):
    def kernel(*refs):
        pick_kernel(sizes, slot, n, *refs)

    return pl.pallas_call(
        kernel,
        out_shape=jax.ShapeDtypeStruct((ROWS * slot, 128), F32),
        in_specs=[pl.BlockSpec(memory_space=SMEM), pl.BlockSpec(memory_space=ANY)],
        scratch_shapes=[VMEM((slot, ROWS + 16, 128), F32), pltpu.SemaphoreType.DMA((slot,))],
        compiler_params=vm(8),
        name="pick",
    )(own_root, parts)


def program(potential, frag_root):
    bx, by, bz = potential.shape
    groups = lax.axis_size("gx")
    zs = lax.axis_size("gz")
    sizes = (bx * groups, by * lax.axis_size("gy"), bz * zs, bx, by, bz)
    slot = frag_root.shape[1]
    place = jnp.stack([lax.axis_index("gx"), lax.axis_index("gy"), lax.axis_index("gz")]).astype(jnp.int32)

    def move(v, sx, sz):
        axis, count, by = ("gx", groups, sx) if sx else ("gz", zs, sz)
        return lax.ppermute(v, axis, [(i, (i + by) % count) for i in range(count)])

    before = move(potential[bx - HALO:], 1, 0)
    after = move(potential[:HALO], -1, 0)
    za, zb = pack(potential)
    got_zb = move(zb, 0, 1)
    got_za = move(za, 0, -1)
    left = move(jnp.concatenate([got_zb[8:], got_za[8:]], axis=0), 1, 0)
    right = move(jnp.concatenate([got_zb[:12], got_za[:12]], axis=0), -1, 0)
    roots = lax.all_to_all(
        jnp.broadcast_to(frag_root[None], (groups, 3, slot)), "gx", 0, 0, tiled=True
    )

    swap = [(0, 1), (1, 0)]
    part_own = lax.ppermute(potential, "gy", swap)
    part_after = lax.ppermute(after, "gy", swap)
    part_before = lax.ppermute(before, "gy", swap)
    full = middle(before, potential, after, part_before, part_own, part_after, zb)
    own_h = halos(got_zb, got_za, left, right, roots)
    part_h = lax.ppermute(own_h, "gy", swap)

    table = interp_matrix()
    hi = np.asarray(table.astype(BF16))
    lo = (table - hi.astype(np.float32)).astype(BF16)
    thi = np.zeros((G, 128), BF16)
    tlo = np.zeros((G, 128), BF16)
    thi[:, :BOX] = hi
    tlo[:, :BOX] = lo
    a2 = np.zeros((2 * G, 144), BF16)
    a2[:G, :BOX] = hi
    a2[:G, 72:72 + BOX] = hi
    a2[G:, :BOX] = lo

    done, full = fields(sizes, slot, groups, roots, place, thi, tlo, a2, full)
    full = join_halo(full, own_h, part_h)
    (done,) = fields(sizes, slot, groups, roots, place, thi, tlo, a2, full, done)
    parts = lax.all_to_all(done, "gx", 0, 0, tiled=True)
    out = pick(sizes, slot, groups, frag_root, parts)
    return jnp.transpose(out.reshape(ROWS, slot, 128), (1, 0, 2)).reshape(slot, ROWS * 128)


def solution(mesh):
    return jax.shard_map(
        program,
        mesh=mesh,
        in_specs=(P("gx", "gy", "gz"), P(None, ("gx", "gy", "gz"))),
        out_specs=P(("gx", "gy", "gz"), None),
        check_vma=False,
    )
```
